32 devices in a mesh: gx: 2 (over x), gy: 4 (over y, core), gz: 4 (over z).
Axes of the slice: x: 2, y: 2, z: 4, core: 2. Of those that a mesh axis runs over, the one named last changes fastest.
Arguments:
- flow_pops: float32 [19, 16, 32, 512], P(None, 'gx', 'gy', 'gz'), may hold values from 0 to 0.6, as said below
- heat_pops: float32 [7, 16, 32, 512], P(None, 'gx', 'gy', 'gz'), may hold values from -0.2 to 0.2
Outputs:
- flow_out: float32 [19, 16, 32, 512], P(None, 'gx', 'gy', 'gz')
- heat_out: float32 [7, 16, 32, 512], P(None, 'gx', 'gy', 'gz')
- nusselt: float32 [], replicated
The draws below stay inside these ranges and needn't reach their ends.
Inputs may be any that keep to these rules, and one draw needn't show every extreme that they name: `flow_pops`: positive flow populations.
All inputs are finite; a program needn't handle non-finite values.
Results may differ from the reference program's by a relative error of at most 0.0001.
Values sent between devices are 32-bit elements; how exact they have to be, the bound alone decides.
A program may use at most 64 MiB of HBM per device.

```python
import jax
import jax.numpy as jnp
import numpy as np

STEPS = 3
NX = 16
NY = 32
NZ = 512


FLOW_WEIGHT = np.array([1.0 / 3.0] + [1.0 / 18.0] * 6 + [1.0 / 36.0] * 12)


D3Q7_QUADRATURE = np.array([0.25] + [0.125] * 6)


def draw_flow_pops(key, part):
    weight = jnp.asarray(FLOW_WEIGHT, jnp.float32).reshape(19, 1, 1, 1)
    factor = jax.random.uniform(key, (19, NX, NY, NZ), jnp.float32, 0.8, 1.2)
    return (weight * factor).astype(jnp.float32)


def draw_heat_pops(key, part):
    weight = jnp.asarray(D3Q7_QUADRATURE, jnp.float32).reshape(7, 1, 1, 1)
    noise = jax.random.uniform(jax.random.fold_in(key, 21), (7, NX, NY, NZ), jnp.float32, -0.1, 0.1)
    cell_temp = jax.random.uniform(jax.random.fold_in(key, 23), (1, NX, NY, NZ), jnp.float32, -0.4, 0.4)
    return (weight * (cell_temp + noise)).astype(jnp.float32)


def setup_inputs(seed: int = 0) -> dict:
    splits = jax.random.split(jax.random.key(seed), 3)
    flow_pops = draw_flow_pops(jax.random.fold_in(splits[2], 71), 0)
    heat_pops = draw_heat_pops(jax.random.fold_in(splits[2], 71), 0)
    return dict(flow_pops=flow_pops, heat_pops=heat_pops)


FLOW_SET = np.array([[0, 0, 0], [1, 0, 0], [-1, 0, 0], [0, 1, 0], [0, -1, 0], [0, 0, 1], [0, 0, -1], [1, 1, 0], [-1, -1, 0], [1, -1, 0], [-1, 1, 0], [1, 0, 1], [-1, 0, -1], [1, 0, -1], [-1, 0, 1], [0, 1, 1], [0, -1, -1], [0, 1, -1], [0, -1, 1]])
FLOW_WEIGHT = np.array([1.0 / 3.0] + [1.0 / 18.0] * 6 + [1.0 / 36.0] * 12)
D3Q7_QUADRATURE = np.array([0.25] + [0.125] * 6)
LATTICE = np.concatenate([FLOW_SET, FLOW_SET[:7]], axis=0)
WEIGHTS = np.concatenate([FLOW_WEIGHT, D3Q7_QUADRATURE])
OPPOSITE = np.array([[r for r in range(19) if (FLOW_SET[r] == -FLOW_SET[q]).all()][0] for q in range(19)] + [19 + [r for r in range(7) if (FLOW_SET[r] == -FLOW_SET[q]).all()][0] for q in range(7)])
TAU_FLOW = 0.6
TAU_HEAT = 0.7
GRAVITY_LIFT = 0.01
HOT_WALL = 0.5
COLD_WALL = -0.5
DIFFUSIVITY = (TAU_HEAT - 0.5) / 4.0


def stacked_subarray(values, count):
    return jnp.asarray(values[:count], jnp.float32).reshape(count, 1, 1, 1)


def hydrodynamic_observables(momentum_populations, energy_populations):
    mass_per_site = jnp.sum(momentum_populations, axis=0)
    site_warmth = jnp.sum(energy_populations, axis=0)
    gravity_direction_push = GRAVITY_LIFT * mass_per_site * site_warmth
    speed_xaxis_component = jnp.sum(stacked_subarray(FLOW_SET[:, 0], 19) * momentum_populations, axis=0) / mass_per_site
    speed_yaxis_component = jnp.sum(stacked_subarray(FLOW_SET[:, 1], 19) * momentum_populations, axis=0) / mass_per_site
    speed_zaxis_component = (jnp.sum(stacked_subarray(FLOW_SET[:, 2], 19) * momentum_populations, axis=0) + 0.5 * gravity_direction_push) / mass_per_site
    return mass_per_site, site_warmth, gravity_direction_push, speed_xaxis_component, speed_yaxis_component, speed_zaxis_component


def collide(momentum_populations, energy_populations):
    mass_per_site, site_warmth, gravity_direction_push, speed_xaxis_component, speed_yaxis_component, speed_zaxis_component = hydrodynamic_observables(momentum_populations, energy_populations)
    dir_z = stacked_subarray(FLOW_SET[:, 2], 19)
    projected_onto_link = stacked_subarray(FLOW_SET[:, 0], 19) * speed_xaxis_component + stacked_subarray(FLOW_SET[:, 1], 19) * speed_yaxis_component + dir_z * speed_zaxis_component
    speed_sq = speed_xaxis_component * speed_xaxis_component + speed_yaxis_component * speed_yaxis_component + speed_zaxis_component * speed_zaxis_component
    weight = stacked_subarray(FLOW_WEIGHT, 19)
    equil = weight * mass_per_site * (1.0 + 3.0 * projected_onto_link + 4.5 * projected_onto_link * projected_onto_link - 1.5 * speed_sq)
    source = (1.0 - 0.5 / TAU_FLOW) * weight * (3.0 * (dir_z - speed_zaxis_component) + 9.0 * projected_onto_link * dir_z) * gravity_direction_push
    flow_post = momentum_populations - (momentum_populations - equil) / TAU_FLOW + source
    warmth_rest_distribution = stacked_subarray(D3Q7_QUADRATURE, 7) * site_warmth * (1.0 + 4.0 * projected_onto_link[:7])
    heat_post = energy_populations - (energy_populations - warmth_rest_distribution) / TAU_HEAT
    return jnp.concatenate([flow_post, heat_post], axis=0)


def apply_walls(read, post, is_bottom, is_top):
    result = []
    for member in range(26):
        single = read[member]
        dir_z = int(LATTICE[member, 2])
        if dir_z != 0:
            plane = 0 if dir_z == 1 else single.shape[2] - 1
            flag = is_bottom if dir_z == 1 else is_top
            wall_temp = HOT_WALL if dir_z == 1 else COLD_WALL
            back = post[int(OPPOSITE[member])][:, :, plane]
            if member >= 19:
                back = -back + 2.0 * float(WEIGHTS[member]) * wall_temp
            single = single.at[:, :, plane].set(jnp.where(flag, back, single[:, :, plane]))
        result.append(single)
    return jnp.stack(result)


def local_flux(momentum_populations, energy_populations):
    mass_per_site, site_warmth, gravity_direction_push, speed_xaxis_component, speed_yaxis_component, speed_zaxis_component = hydrodynamic_observables(momentum_populations, energy_populations)
    return jnp.sum(speed_zaxis_component * site_warmth)


def reference(flow_pops, heat_pops):
    momentum_populations, energy_populations = flow_pops, heat_pops
    for period in range(STEPS):
        post = collide(momentum_populations, energy_populations)
        result = []
        for member in range(26):
            single = jnp.roll(post[member], int(LATTICE[member, 0]), 0)
            single = jnp.roll(single, int(LATTICE[member, 1]), 1)
            dir_z = int(LATTICE[member, 2])
            zeros = jnp.zeros(single.shape[:2] + (1,), jnp.float32)
            if dir_z == 1:
                single = jnp.concatenate([zeros, single[:, :, :-1]], axis=2)
            elif dir_z == -1:
                single = jnp.concatenate([single[:, :, 1:], zeros], axis=2)
            result.append(single)
        read = apply_walls(jnp.stack(result), post, True, True)
        momentum_populations, energy_populations = read[:19], read[19:]
    total = local_flux(momentum_populations, energy_populations)
    nusselt = 1.0 + NZ / (DIFFUSIVITY * (HOT_WALL - COLD_WALL)) * total / (NX * NY * NZ)
    return momentum_populations, energy_populations, nusselt.astype(jnp.float32)
```

```python
import functools

import jax
import jax.numpy as jnp
import numpy as np
from jax import lax
from jax.experimental import pallas as pl
from jax.experimental.pallas import tpu as pltpu
from jax.sharding import PartitionSpec as P

STEPS = 3

FLOW_SET = np.array(
    [
        [0, 0, 0],
        [1, 0, 0],
        [-1, 0, 0],
        [0, 1, 0],
        [0, -1, 0],
        [0, 0, 1],
        [0, 0, -1],
        [1, 1, 0],
        [-1, -1, 0],
        [1, -1, 0],
        [-1, 1, 0],
        [1, 0, 1],
        [-1, 0, -1],
        [1, 0, -1],
        [-1, 0, 1],
        [0, 1, 1],
        [0, -1, -1],
        [0, 1, -1],
        [0, -1, 1],
    ]
)
FLOW_WEIGHT = np.array([1.0 / 3.0] + [1.0 / 18.0] * 6 + [1.0 / 36.0] * 12)
HEAT_WEIGHT = np.array([0.25] + [0.125] * 6)
LATTICE = [tuple(int(c) for c in v) for v in np.concatenate([FLOW_SET, FLOW_SET[:7]], axis=0)]
WEIGHTS = [float(w) for w in np.concatenate([FLOW_WEIGHT, HEAT_WEIGHT])]
OPPOSITE = (
    [0]
    + [q + 1 if q % 2 else q - 1 for q in range(1, 19)]
    + [19]
    + [q - 1 if q % 2 else q + 1 for q in range(20, 26)]
)
TAU_FLOW = 0.6
TAU_HEAT = 0.7
GRAVITY_LIFT = 0.01
HOT_WALL = 0.5
COLD_WALL = -0.5
DIFFUSIVITY = (TAU_HEAT - 0.5) / 4.0

MEMBERS = {
    (axis, sign): [q for q in range(26) if LATTICE[q][axis] == sign]
    for axis in range(3)
    for sign in (1, -1)
}
FACE = len(MEMBERS[0, 1])
STORED = (
    MEMBERS[0, 1] + MEMBERS[0, -1] + [q for q in range(26) if LATTICE[q][0] == 0]
)
SLOT = [STORED.index(q) for q in range(26)]
SIDES = (1, -1)
UNROLL = 3
LINKS = sorted({v for v in LATTICE if v != (0, 0, 0)})


def side(sign):
    return 0 if sign == 1 else 1


def moments(f, g):
    rho = functools.reduce(lambda a, b: a + b, f)
    warmth = functools.reduce(lambda a, b: a + b, g)
    flow = []
    for axis in range(3):
        total = None
        for q in range(1, 19, 2):
            if LATTICE[q][axis]:
                odd = f[q] - f[q + 1]
                if total is None:
                    total = odd
                else:
                    total = total + odd if LATTICE[q][axis] == 1 else total - odd
        flow.append(total)
    push = GRAVITY_LIFT * rho * warmth
    inv = 1.0 / rho
    return (rho, warmth, push, flow[0] * inv, flow[1] * inv, (flow[2] + 0.5 * push) * inv)


def collide(f, g):
    rho, warmth, push, ux, uy, uz = moments(f, g)
    rate = 1.0 / TAU_FLOW
    lift = 1.0 - 0.5 / TAU_FLOW
    keep = 1.0 - rate
    base = (rate * rho) * (1.0 - 1.5 * (ux * ux + uy * uy + uz * uz)) - (3.0 * lift) * uz * push
    quad = (4.5 * rate) * rho
    line = (3.0 * rate) * rho
    push3 = (3.0 * lift) * push
    push9 = (9.0 * lift) * push
    post = [None] * 26
    post[0] = keep * f[0] + WEIGHTS[0] * base
    u = (ux, uy, uz)
    for q in range(1, 19, 2):
        c = LATTICE[q]
        along = None
        for axis in range(3):
            if c[axis]:
                if along is None:
                    along = u[axis]
                else:
                    along = along + u[axis] if c[axis] == 1 else along - u[axis]
        inner = quad * along
        odd = line * along
        if c[2] == 1:
            inner, odd = inner + push9, odd + push3
        elif c[2] == -1:
            inner, odd = inner - push9, odd - push3
        even = WEIGHTS[q] * (base + along * inner)
        odd = WEIGHTS[q] * odd
        post[q] = keep * f[q] + (even + odd)
        post[q + 1] = keep * f[q + 1] + (even - odd)
    heat_rate = 1.0 / TAU_HEAT
    heat_keep = 1.0 - heat_rate
    post[19] = heat_keep * g[0] + (WEIGHTS[19] * heat_rate) * warmth
    still = (WEIGHTS[20] * heat_rate) * warmth
    for axis in range(3):
        drift = (4.0 * WEIGHTS[20] * heat_rate) * warmth * u[axis]
        q = 20 + 2 * axis
        post[q] = heat_keep * g[q - 19] + (still + drift)
        post[q + 1] = heat_keep * g[q - 18] + (still - drift)
    return post


def kernel(
    sizes, flow_in, heat_in, result,
    cur, post, sy, ry, sz, rz, syz, ryz, sums,
    in_sem, send_sem, recv_sem, sum_send, sum_recv,
):
    count_x, count_y, count_z = sizes
    nx, ny, nz = cur.shape[1:]
    gx, gy, gz = (lax.axis_index(a) for a in ("gx", "gy", "gz"))
    has = {1: gz < count_z - 1, -1: gz > 0}
    everyone = count_x * count_y * count_z
    me = (gx * count_y + gy) * count_z + gz

    def device(v):
        return {
            "gx": lax.rem(gx + v[0] + count_x, count_x),
            "gy": lax.rem(gy + v[1] + count_y, count_y),
            "gz": gz + v[2],
        }

    def ahead(distance):
        other = lax.rem(me + distance, everyone)
        row = other // count_z
        return {"gx": row // count_y, "gy": lax.rem(row, count_y), "gz": lax.rem(other, count_z)}

    def load(x):
        return (
            pltpu.make_async_copy(flow_in.at[:, x], cur.at[0:19, x], in_sem.at[0, x]),
            pltpu.make_async_copy(heat_in.at[:, x], cur.at[19:26, x], in_sem.at[1, x]),
        )

    for x in [0, nx - 1] + list(range(1, nx - 1)):
        for copy in load(x):
            copy.start()

    barrier = pltpu.get_barrier_semaphore()
    near = sorted({(v[0] % count_x, v[1] % count_y, v[2]) for v in LINKS})
    reach = (count_x // 2, count_y // 2, count_z - 1)
    joined = max(reach) <= STEPS and sum(reach) <= 2 * STEPS
    if joined:
        for v in near:
            if v[2] == 0:
                pl.semaphore_signal(barrier, inc=1, device_id=device(v))
        for sign in SIDES:
            @pl.when(has[sign])
            def _():
                for v in near:
                    if v[2] == sign:
                        pl.semaphore_signal(barrier, inc=1, device_id=device(v))
    else:
        @pl.loop(1, everyone)
        def _(d):
            pl.semaphore_signal(barrier, inc=1, device_id=ahead(d))

    def greet():
        if joined:
            count = len([v for v in near if v[2] == 0])
            for sign in SIDES:
                count += jnp.where(has[sign], len([v for v in near if v[2] == sign]), 0)
        else:
            count = everyone - 1
        pl.semaphore_wait(barrier, count)

    lane = lax.broadcasted_iota(jnp.int32, (ny, nz), 1)
    row = lax.broadcasted_iota(jnp.int32, (ny, nz), 0)
    first_row, last_row = row == 0, row == ny - 1
    first_lane, last_lane = lane == 0, lane == nz - 1

    def message(s, v):
        i = LINKS.index(v)
        x, y, z = v
        if z == 0:
            start = 0 if x == 1 else FACE
            edge, halo = (nx, 0) if x == 1 else (1, nx + 1)
            if y == 0:
                src = post.at[s, start : start + FACE, edge]
                dst = post.at[s, start : start + FACE, halo]
            elif x == 0:
                src = sy.at[s, side(y), :, 1 : nx + 1]
                dst = ry.at[s, side(y), :, 1 : nx + 1]
            else:
                j = MEMBERS[1, y].index(LATTICE.index(v))
                src = sy.at[s, side(y), j, edge]
                dst = ry.at[s, side(y), j, halo]
        elif y == 0:
            src = sz.at[s, side(z), 0 if x == 0 else 1]
            dst = rz.at[s, side(z), 0 if x == 0 else 1 + side(x)]
        else:
            src = syz.at[s, side(z), side(y)]
            dst = ryz.at[s, side(z), side(y)]
        return pltpu.make_async_remote_copy(
            src_ref=src, dst_ref=dst, send_sem=send_sem.at[s, i], recv_sem=recv_sem.at[s, i],
            device_id=device(v),
        )

    def send(s, links):
        for sign in SIDES:
            @pl.when(has[sign])
            def _():
                for v in links:
                    if v[2] == sign:
                        message(s, v).start()
        for v in links:
            if v[2] == 0:
                message(s, v).start()

    def receive(s):
        for v in LINKS:
            if v[2] == 0:
                message(s, v).wait_recv()
        for sign in SIDES:
            @pl.when(has[-sign])
            def _():
                for v in LINKS:
                    if v[2] == sign:
                        message(s, v).wait_recv()

    hops = lambda v: -sum(abs(c) for c in v)
    early = sorted([v for v in LINKS if v[0]], key=hops)
    late = sorted([v for v in LINKS if not v[0]], key=hops)
    width = FACE

    def keep_plane(s, x, values, packs):
        for q in range(26):
            post[s, SLOT[q], x + 1] = values[q]
        for sign in SIDES:
            r = ny - 1 if sign == 1 else 0
            for j, q in enumerate(MEMBERS[1, sign]):
                sy[s, side(sign), j, x + 1] = values[q][r : r + 1, :]
        new = []
        for sign, pack in zip(SIDES, packs):
            source = nz - 1 if sign == 1 else 0
            part = None
            for j, q in enumerate(MEMBERS[2, sign]):
                turned = pltpu.roll(values[q], (j - source) % nz, 1)
                part = turned if part is None else jnp.where(lane == j, turned, part)
            base = (x + 1) * width
            part = pltpu.roll(part, base, 1)
            new.append(jnp.where((lane >= base) & (lane < base + width), part, pack))
        return tuple(new)

    def run_planes(s, body):
        zero = jnp.zeros((ny, nz), jnp.float32)
        packs = lax.fori_loop(
            0, 2, lambda i, p: keep_plane(s, i * (nx - 1), body(i * (nx - 1)), p), (zero, zero), unroll=True
        )
        return packs

    def advance(s, body, before_send):
        packs = run_planes(s, body)
        for sign, pack in zip(SIDES, packs):
            sz[s, side(sign), 1] = pack
        before_send()
        send(s, early)
        packs = lax.fori_loop(
            1, nx - 1, lambda x, p: keep_plane(s, x, body(x), p), packs, unroll=UNROLL
        )
        for sign, pack in zip(SIDES, packs):
            sz[s, side(sign), 0] = pack
            for sign_y in SIDES:
                r = ny - 1 if sign_y == 1 else 0
                syz[s, side(sign), side(sign_y)] = pack[r : r + 1, :]
        send(s, late)

    def columns(s):
        result = {}
        for sign in SIDES:
            straight = rz[s, side(sign), 0]
            low = pltpu.roll(rz[s, side(sign), 1], (-nx * width) % nz, 1)
            high = pltpu.roll(rz[s, side(sign), 2], (nx * width) % nz, 1)
            result[sign, 0] = jnp.where(
                lane < width, low, jnp.where(lane >= (nx + 1) * width, high, straight)
            )
            for sign_y in SIDES:
                turned = pltpu.roll(straight, sign_y % ny, 0)
                edge = jnp.broadcast_to(ryz[s, side(sign), side(sign_y)], (ny, nz))
                result[sign, sign_y] = jnp.where(
                    first_row if sign_y == 1 else last_row, edge, turned
                )
        return result

    def pull(s, x, beyond, q):
        cx, cy, cz = LATTICE[q]
        at = x - cx + 1
        value = post[s, SLOT[q], at]
        if cy:
            j = MEMBERS[1, cy].index(q)
            edge = jnp.broadcast_to(ry[s, side(cy), j, at], (ny, nz))
            value = jnp.where(
                first_row if cy == 1 else last_row, edge, pltpu.roll(value, cy % ny, 0)
            )
        if cz:
            j = MEMBERS[2, cz].index(q)
            target = 0 if cz == 1 else nz - 1
            outer = pltpu.roll(beyond[cz, cy], lax.rem(target - (at * width + j) + nz, nz), 1)
            back = post[s, SLOT[OPPOSITE[q]], x + 1]
            if q >= 19:
                back = 2.0 * WEIGHTS[q] * (HOT_WALL if cz == 1 else COLD_WALL) - back
            outer = jnp.where(has[-cz], outer, back)
            value = jnp.where(
                first_lane if cz == 1 else last_lane, outer, pltpu.roll(value, cz % nz, 1)
            )
        return value

    def fresh(x):
        for copy in load(x):
            copy.wait()
        return collide([cur[q, x] for q in range(19)], [cur[q, x] for q in range(19, 26)])

    advance(0, fresh, greet)

    def step(s, carry):
        receive(s)
        beyond = columns(s)

        def body(x):
            values = [pull(s, x, beyond, q) for q in range(26)]
            return collide(values[:19], values[19:])

        advance(s + 1, body, lambda: None)
        return carry

    lax.fori_loop(0, STEPS - 1, step, 0)

    last = STEPS - 1
    receive(last)
    beyond = columns(last)

    def finish(x, total):
        values = [pull(last, x, beyond, q) for q in range(26)]
        for q in range(19):
            result[q, x] = values[q]
        for q in range(7):
            result[19 + q, x] = values[19 + q]
        _, warmth, _, _, _, uz = moments(values[:19], values[19:])
        return total + uz * warmth

    total = lax.fori_loop(0, nx, finish, jnp.zeros((ny, nz), jnp.float32), unroll=4)
    sums[me] = jnp.sum(total, axis=0, keepdims=True)

    def send_sum(target):
        pltpu.make_async_remote_copy(
            src_ref=sums.at[me], dst_ref=sums.at[me],
            send_sem=sum_send, recv_sem=sum_recv, device_id=target,
        ).start()

    if joined:
        xs, ys, zs = (
            [lax.rem(at + d, n) for d in range(n)] for at, n in zip((gx, gy, gz), sizes)
        )
        for dz in reversed(range(count_z)):
            for dx in reversed(range(count_x)):
                for dy in reversed(range(count_y)):
                    if dx or dy or dz:
                        send_sum({"gx": xs[dx], "gy": ys[dy], "gz": zs[dz]})
    else:
        pl.loop(1, everyone)(lambda d: send_sum(ahead(d)))

    for s in range(STEPS):
        for v in LINKS:
            if v[2] == 0:
                message(s, v).wait_send()
        for sign in SIDES:
            @pl.when(has[sign])
            def _():
                for v in LINKS:
                    if v[2] == sign:
                        message(s, v).wait_send()
    all_rows = pltpu.make_async_remote_copy(
        src_ref=sums.at[pl.ds(0, everyone - 1)], dst_ref=sums.at[pl.ds(0, everyone - 1)],
        send_sem=sum_send, recv_sem=sum_recv, device_id=ahead(1),
    )
    all_rows.wait_send()
    all_rows.wait_recv()
    cells = nx * ny * nz * count_x * count_y * count_z
    scale = nz * count_z / (DIFFUSIVITY * (HOT_WALL - COLD_WALL)) / cells
    result[26, 0, 0:1, :] = jnp.full((1, nz), 1.0 + scale * jnp.sum(jnp.sum(sums[...], axis=0)))


def write_out(result, flow_out, heat_out, nusselt_out, small, sem):
    small[...] = result[26, 0, 0:1, 0:1]
    copies = []
    for q in range(0, 19, 2):
        n = min(2, 19 - q)
        copies.append(pltpu.make_async_copy(result.at[q : q + n], flow_out.at[q : q + n], sem.at[q]))
    for q in range(0, 7, 2):
        n = min(2, 7 - q)
        copies.append(pltpu.make_async_copy(result.at[19 + q : 19 + q + n], heat_out.at[q : q + n], sem.at[19 + q]))
    copies.append(pltpu.make_async_copy(small, nusselt_out, sem.at[26]))
    for copy in copies:
        copy.start()
    for copy in copies:
        copy.wait()


def per_device(sizes, flow_pops, heat_pops):
    nx, ny, nz = flow_pops.shape[1:]
    count_x, count_y, count_z = sizes
    f32 = jnp.float32
    dma = pltpu.SemaphoreType.DMA
    hbm = pl.BlockSpec(memory_space=pltpu.HBM)
    vmem = pl.BlockSpec(memory_space=pltpu.VMEM)
    result = pl.pallas_call(
        functools.partial(kernel, sizes),
        out_shape=pltpu.VMEM((27, nx, ny, nz), f32),
        in_specs=[hbm, hbm],
        out_specs=vmem,
        scratch_shapes=[
            pltpu.VMEM((26, nx, ny, nz), f32),
            pltpu.VMEM((STEPS, 26, nx + 2, ny, nz), f32),
            pltpu.VMEM((STEPS, 2, FACE, nx + 2, 1, nz), f32),
            pltpu.VMEM((STEPS, 2, FACE, nx + 2, 1, nz), f32),
            pltpu.VMEM((STEPS, 2, 2, ny, nz), f32),
            pltpu.VMEM((STEPS, 2, 3, ny, nz), f32),
            pltpu.VMEM((STEPS, 2, 2, 1, nz), f32),
            pltpu.VMEM((STEPS, 2, 2, 1, nz), f32),
            pltpu.VMEM((count_x * count_y * count_z, 1, nz), f32),
            dma((2, nx)),
            dma((STEPS, len(LINKS))),
            dma((STEPS, len(LINKS))),
            dma,
            dma,
        ],
        compiler_params=pltpu.CompilerParams(
            collective_id=0, has_side_effects=True, vmem_limit_bytes=55000000
        ),
    )(pltpu.with_memory_space_constraint(flow_pops, pltpu.HBM), pltpu.with_memory_space_constraint(heat_pops, pltpu.HBM))
    flow, heat, nusselt = pl.pallas_call(
        write_out,
        out_shape=(
            jax.ShapeDtypeStruct(flow_pops.shape, f32),
            jax.ShapeDtypeStruct(heat_pops.shape, f32),
            jax.ShapeDtypeStruct((1, 1), f32),
        ),
        in_specs=[vmem],
        out_specs=(hbm, hbm, hbm),
        scratch_shapes=[pltpu.VMEM((1, 1), f32), dma((27,))],
        compiler_params=pltpu.CompilerParams(vmem_limit_bytes=1024 * 1024),
    )(result)
    return flow, heat, nusselt.reshape(())


def solution(mesh):
    placed = P(None, "gx", "gy", "gz")
    sizes = tuple(mesh.shape[a] for a in ("gx", "gy", "gz"))
    return jax.shard_map(
        functools.partial(per_device, sizes),
        mesh=mesh,
        in_specs=(placed, placed),
        out_specs=(placed, placed, P()),
        check_vma=False,
    )
```

```python
import functools

import jax
import jax.numpy as jnp
import numpy as np
from jax import lax
from jax.experimental import pallas as pl
from jax.experimental.pallas import tpu as pltpu
from jax.sharding import PartitionSpec as P

STEPS = 3

FLOW_SET = np.array(
    [
        [0, 0, 0],
        [1, 0, 0],
        [-1, 0, 0],
        [0, 1, 0],
        [0, -1, 0],
        [0, 0, 1],
        [0, 0, -1],
        [1, 1, 0],
        [-1, -1, 0],
        [1, -1, 0],
        [-1, 1, 0],
        [1, 0, 1],
        [-1, 0, -1],
        [1, 0, -1],
        [-1, 0, 1],
        [0, 1, 1],
        [0, -1, -1],
        [0, 1, -1],
        [0, -1, 1],
    ]
)
FLOW_WEIGHT = np.array([1.0 / 3.0] + [1.0 / 18.0] * 6 + [1.0 / 36.0] * 12)
HEAT_WEIGHT = np.array([0.25] + [0.125] * 6)
LATTICE = [tuple(int(c) for c in v) for v in np.concatenate([FLOW_SET, FLOW_SET[:7]], axis=0)]
WEIGHTS = [float(w) for w in np.concatenate([FLOW_WEIGHT, HEAT_WEIGHT])]
OPPOSITE = (
    [0]
    + [q + 1 if q % 2 else q - 1 for q in range(1, 19)]
    + [19]
    + [q - 1 if q % 2 else q + 1 for q in range(20, 26)]
)
TAU_FLOW = 0.6
TAU_HEAT = 0.7
GRAVITY_LIFT = 0.01
HOT_WALL = 0.5
COLD_WALL = -0.5
DIFFUSIVITY = (TAU_HEAT - 0.5) / 4.0
KEEP_FLOW = 1.0 - 1.0 / TAU_FLOW
KEEP_HEAT = 1.0 - 1.0 / TAU_HEAT

MEMBERS = {
    (axis, sign): [q for q in range(26) if LATTICE[q][axis] == sign]
    for axis in range(3)
    for sign in (1, -1)
}
FACE = len(MEMBERS[0, 1])
STORED = (
    MEMBERS[0, 1] + MEMBERS[0, -1] + [q for q in range(26) if LATTICE[q][0] == 0]
)
SLOT = [STORED.index(q) for q in range(26)]
SIDES = (1, -1)
UNROLL = True
LINKS = sorted({v for v in LATTICE if v != (0, 0, 0)})


EARLY = sorted([v for v in LINKS if v[0]], key=lambda v: sum(abs(c) for c in v))
LATE = sorted([v for v in LINKS if not v[0]], key=lambda v: -sum(abs(c) for c in v))


def group(v):
    return 0 if v[2] == 0 else 1 + side(v[2])


def side(sign):
    return 0 if sign == 1 else 1


def total(terms):
    terms = list(terms)
    while len(terms) > 1:
        terms = [a + b for a, b in zip(terms[::2], terms[1::2])] + terms[len(terms) & ~1 :]
    return terms[0]


def gather(values, span):
    flat = [values[q - span[0]] for q in span if LATTICE[q][2] == 0]
    tilted = [values[q - span[0]] for q in span if LATTICE[q][2]]
    return total(flat) + total(tilted)


def moments(f, g, scale):
    rho, warmth = gather(f, range(19)), gather(g, range(19, 26))
    flow = []
    for axis in range(3):
        result = None
        for q in sorted(range(1, 19, 2), key=lambda q: abs(LATTICE[q][2])):
            if LATTICE[q][axis]:
                odd = f[q] - f[q + 1]
                if result is None:
                    result = odd
                else:
                    result = result + odd if LATTICE[q][axis] == 1 else result - odd
        flow.append(result)
    half = (0.5 * GRAVITY_LIFT * scale) * warmth
    inv = 1.0 / rho
    return rho, warmth, half, (flow[0] * inv, flow[1] * inv, flow[2] * inv + half)


def collide(f, g, scale):
    rho, warmth, half, u = moments(f, g, scale)
    push = rho * half
    rate = 1.0 / TAU_FLOW
    lift = 2.0 * (1.0 - 0.5 / TAU_FLOW)
    weight = WEIGHTS[7] / KEEP_FLOW
    square = u[0] * u[0] + u[1] * u[1] + u[2] * u[2]
    base = (weight * rate * rho) * (1.0 - 1.5 * square) - (3.0 * lift * weight) * (u[2] * push)
    quad = (4.5 * rate * weight) * rho
    line = (3.0 * rate * weight) * rho
    push3 = (3.0 * lift * weight) * push
    push9 = (9.0 * lift * weight) * push
    small = (base, quad, line, push3, push9)
    large = tuple((WEIGHTS[1] / WEIGHTS[7]) * part for part in small)
    post = [None] * 26
    post[0] = f[0] + (WEIGHTS[0] / WEIGHTS[7]) * base
    for q in range(1, 19, 2):
        c = LATTICE[q]
        along = None
        for axis in range(3):
            if c[axis]:
                if along is None:
                    along = u[axis]
                else:
                    along = along + u[axis] if c[axis] == 1 else along - u[axis]
        base, quad, line, push3, push9 = large if q < 7 else small
        inner = quad * along
        odd = line * along
        if c[2] == 1:
            inner, odd = inner + push9, odd + push3
        elif c[2] == -1:
            inner, odd = inner - push9, odd - push3
        even = base + along * inner
        post[q] = f[q] + (even + odd)
        post[q + 1] = f[q + 1] + (even - odd)
    share = 1.0 / (TAU_HEAT * KEEP_HEAT)
    post[19] = g[0] + (WEIGHTS[19] * share) * warmth
    still = (WEIGHTS[20] * share) * warmth
    slope = (4.0 * WEIGHTS[20] * share) * warmth
    for axis in range(3):
        drift = slope * u[axis]
        q = 20 + 2 * axis
        post[q] = g[q - 19] + (still + drift)
        post[q + 1] = g[q - 18] + (still - drift)
    return post


def kernel(
    sizes, flow_in, heat_in, result,
    cur, post, mid, sy, ry, sz, rz, syz, ryz, sums, ledger,
    in_sem, send_sem, recv_sem, sum_send, sum_recv,
):
    count_x, count_y, count_z = sizes
    nx, ny, nz = cur.shape[1:]
    gx, gy, gz = (lax.axis_index(a) for a in ("gx", "gy", "gz"))
    has = {1: gz < count_z - 1, -1: gz > 0}
    everyone = count_x * count_y * count_z
    me = (gx * count_y + gy) * count_z + gz

    def device(v):
        return {
            "gx": lax.rem(gx + v[0] + count_x, count_x),
            "gy": lax.rem(gy + v[1] + count_y, count_y),
            "gz": gz + v[2],
        }

    def ahead(distance):
        other = lax.rem(me + distance, everyone)
        row = other // count_z
        return {"gx": row // count_y, "gy": lax.rem(row, count_y), "gz": lax.rem(other, count_z)}

    def load(part, x):
        return (
            pltpu.make_async_copy(flow_in.at[:, x], cur.at[0:19, x], in_sem.at[part]),
            pltpu.make_async_copy(heat_in.at[:, x], cur.at[19:26, x], in_sem.at[part]),
        )

    loads = [load(0, 0), load(1, nx - 1), [c for x in range(1, nx - 1) for c in load(2, x)]]
    for copies in loads:
        for copy in copies:
            copy.start()

    barrier = pltpu.get_barrier_semaphore()
    near = sorted({(v[0] % count_x, v[1] % count_y, v[2]) for v in LINKS})
    reach = (count_x // 2, count_y // 2, count_z - 1)
    joined = max(reach) <= STEPS and sum(reach) <= 2 * STEPS
    if joined:
        for v in near:
            if v[2] == 0:
                pl.semaphore_signal(barrier, inc=1, device_id=device(v))
        for sign in SIDES:
            @pl.when(has[sign])
            def _():
                for v in near:
                    if v[2] == sign:
                        pl.semaphore_signal(barrier, inc=1, device_id=device(v))
    else:
        @pl.loop(1, everyone)
        def _(d):
            pl.semaphore_signal(barrier, inc=1, device_id=ahead(d))

    def greet():
        if joined:
            count = len([v for v in near if v[2] == 0])
            for sign in SIDES:
                count += jnp.where(has[sign], len([v for v in near if v[2] == sign]), 0)
        else:
            count = everyone - 1
        pl.semaphore_wait(barrier, count)

    lane = lax.broadcasted_iota(jnp.int32, (ny, nz), 1)
    row = lax.broadcasted_iota(jnp.int32, (ny, nz), 0)
    first_row, last_row = row == 0, row == ny - 1
    first_lane, last_lane = lane == 0, lane == nz - 1
    place = lax.rem(lane, FACE)

    def lanes_of(sign, pick):
        mask = None
        for j, q in enumerate(MEMBERS[2, sign]):
            if pick(q):
                mask = place == j if mask is None else mask | (place == j)
        return mask

    def message(s, v):
        x, y, z = v
        if z == 0:
            start = 0 if x == 1 else FACE
            edge, halo = (nx, 0) if x == 1 else (1, nx + 1)
            if y == 0:
                src = post.at[s, start : start + FACE, edge]
                dst = post.at[s, start : start + FACE, halo]
            elif x == 0:
                src = sy.at[s, side(y), :, 1 : nx + 1]
                dst = ry.at[s, side(y), :, 1 : nx + 1]
            else:
                j = MEMBERS[1, y].index(LATTICE.index(v))
                src = sy.at[s, side(y), j, edge]
                dst = ry.at[s, side(y), j, halo]
        elif y == 0:
            src = sz.at[s, side(z), 0 if x == 0 else 1]
            dst = rz.at[s, side(z), 0 if x == 0 else 1 + side(x)]
        else:
            src = syz.at[s, side(z), side(y)]
            dst = ryz.at[s, side(z), side(y)]
        return pltpu.make_async_remote_copy(
            src_ref=src, dst_ref=dst, send_sem=send_sem.at[group(v)], recv_sem=recv_sem.at[s, group(v)],
            device_id=device(v),
        )

    def send(s, links):
        for v in links:
            if v[2] == 0:
                message(s, v).start()
        for sign in SIDES:
            if any(v[2] == sign for v in links):
                @pl.when(has[sign])
                def _():
                    for v in links:
                        if v[2] == sign:
                            message(s, v).start()

    def rows(links):
        count = 0
        for x, y, z in links:
            if y == 0:
                count += FACE * ny if z == 0 else ny
            else:
                count += FACE * nx if x == 0 and z == 0 else 1
        return count

    def settle(sem, count):
        pltpu.make_async_copy(ledger.at[0:count], ledger.at[0:count], sem).wait()

    def receive(s):
        settle(recv_sem.at[s, 0], rows(v for v in LINKS if v[2] == 0))
        for sign in SIDES:
            @pl.when(has[-sign])
            def _():
                settle(recv_sem.at[s, 1 + side(sign)], rows(v for v in LINKS if v[2] == sign))

    def target(x, q):
        return lax.rem(x + (LATTICE[q][0] + nx), nx) * FACE

    def keep_plane(s, x, values, packs):
        for q in range(26):
            post[s, SLOT[q], x + 1] = values[q]
        for sign in SIDES:
            r = ny - 1 if sign == 1 else 0
            for j, q in enumerate(MEMBERS[1, sign]):
                value = values[q]
                if LATTICE[q][2]:
                    value = pltpu.roll(value, LATTICE[q][2] % nz, 1)
                sy[s, side(sign), j, x + 1] = value[r : r + 1, :]
        new = []
        for sign, pack in zip(SIDES, packs):
            source = nz - 1 if sign == 1 else 0
            for j, q in enumerate(MEMBERS[2, sign]):
                k = target(x, q) + j
                turned = pltpu.roll(values[q], lax.rem(k + (nz - source), nz), 1)
                pack = jnp.where(lane == k, turned, pack)
            new.append(pack)
        return tuple(new)

    def stream(s, x):
        for q in range(26):
            cx, cy, cz = LATTICE[q]
            if cy or cz:
                value = post[s, SLOT[q], x + 1]
                if cz:
                    value = pltpu.roll(value, cz % nz, 1)
                if cy:
                    value = pltpu.roll(value, cy % ny, 0)
                mid[SLOT[q], x] = value

    def bounce(s, sign, pack, unit):
        own = MEMBERS[2, sign]
        edge = (nx - 1) * FACE
        wall = pack
        for x in SIDES:
            near_part = pltpu.roll(pack, (-x * FACE) % nz, 1)
            far_part = pltpu.roll(pack, (x * edge) % nz, 1)
            far = lane >= edge if x == 1 else lane < FACE
            wall = jnp.where(
                lanes_of(sign, lambda q: LATTICE[q][0] == x), jnp.where(far, far_part, near_part), wall
            )
        for y in SIDES:
            wall = jnp.where(
                lanes_of(sign, lambda q: LATTICE[q][1] == y), pltpu.roll(pack, -y % ny, 0), wall
            )
        weight = WEIGHTS[own[-1]]
        warm = (2.0 * weight * (COLD_WALL if sign == 1 else HOT_WALL)) * unit
        rz[s, side(-sign), 0] = jnp.where(lanes_of(sign, lambda q: q >= 19), warm - wall, wall)

    def arrive():
        planes = ((0, cur.at[:, 0]), (1, cur.at[:, nx - 1]), (2, cur.at[:, 1 : nx - 1]))
        for part, planes_of in planes:
            pltpu.make_async_copy(planes_of, planes_of, in_sem.at[part]).wait()
            if part:
                yield

    def advance(s, body, arrive, before_send, unit):
        zero = jnp.zeros((ny, nz), jnp.float32)
        packs = (zero, zero)
        stages = iter(arrive() or ())
        next(stages, None)
        for x in (0, nx - 1):
            packs = keep_plane(s, x, body(x, x), packs)
        before_send()
        send(s, [v for v in EARLY if v[2] == 0])
        for sign, pack in zip(SIDES, packs):
            sz[s, side(sign), 1] = pack
        send(s, [v for v in EARLY if v[2]])
        next(stages, None)
        packs = lax.fori_loop(
            1, nx - 1, lambda x, p: keep_plane(s, x, body(x, None), p), packs, unroll=UNROLL
        )
        send(s, [v for v in LATE if v[2] == 0])
        for sign, pack in zip(SIDES, packs):
            whole = pack
            for y in SIDES:
                whole = jnp.where(
                    lanes_of(sign, lambda q: LATTICE[q][1] == y), pltpu.roll(pack, y % ny, 0), whole
                )
            sz[s, side(sign), 0] = whole
            for y in SIDES:
                r = 0 if y == 1 else ny - 1
                syz[s, side(sign), side(y)] = whole[r : r + 1, :]
        send(s, [v for v in LATE if v[2]])
        for sign in SIDES:
            @pl.when(jnp.logical_not(has[sign]))
            def _():
                bounce(s, sign, sz[s, side(sign), 0], unit)
        lax.fori_loop(0, nx, lambda x, c: (stream(s, x), c)[1], 0, unroll=2)

    def columns(s):
        result = {}
        for sign in SIDES:
            tile = rz[s, side(sign), 0]
            for x in SIDES:
                j = [q for q in MEMBERS[2, sign] if LATTICE[q][0] == x]
                k = (0 if x == 1 else nx - 1) * FACE + MEMBERS[2, sign].index(j[0])
                tile = jnp.where((lane == k) & has[-sign], rz[s, side(sign), 1 + side(x)], tile)
            for y in SIDES:
                mask = lanes_of(sign, lambda q: LATTICE[q][1] == y) & (first_row if y == 1 else last_row)
                edge = jnp.broadcast_to(ryz[s, side(sign), side(y)], (ny, nz))
                tile = jnp.where(mask & has[-sign], edge, tile)
            result[sign] = tile
        return result

    def pull(s, x, fixed, beyond, q):
        cx, cy, cz = LATTICE[q]
        at = x - cx + 1
        if fixed is not None and fixed - cx in (-1, nx):
            value = post[s, SLOT[q], at]
            if cz:
                value = pltpu.roll(value, cz % nz, 1)
            if cy:
                value = pltpu.roll(value, cy % ny, 0)
        elif cy or cz:
            value = mid[SLOT[q], at - 1]
        else:
            value = post[s, SLOT[q], at]
        if cy:
            j = MEMBERS[1, cy].index(q)
            edge = jnp.broadcast_to(ry[s, side(cy), j, at], (ny, nz))
            value = jnp.where(first_row if cy == 1 else last_row, edge, value)
        if cz:
            j = MEMBERS[2, cz].index(q)
            end = 0 if cz == 1 else nz - 1
            outer = pltpu.roll(beyond[cz], lax.rem(end + nz - (x * FACE + j), nz), 1)
            value = jnp.where(first_lane if cz == 1 else last_lane, outer, value)
        return value

    def fresh(x, fixed):
        return collide([cur[q, x] for q in range(19)], [cur[q, x] for q in range(19, 26)], 1.0)

    advance(0, fresh, arrive, greet, 1.0 / KEEP_HEAT)

    def step(s, carry):
        scale, unit = carry
        receive(s)
        beyond = columns(s)

        def body(x, fixed):
            values = [pull(s, x, fixed, beyond, q) for q in range(26)]
            return collide(values[:19], values[19:], scale)

        unit = unit * (1.0 / KEEP_HEAT)
        advance(s + 1, body, lambda: None, lambda: None, unit)
        return scale * KEEP_HEAT, unit

    lax.fori_loop(0, STEPS - 1, step, (jnp.float32(KEEP_HEAT), jnp.float32(1.0 / KEEP_HEAT)))

    last = STEPS - 1
    receive(last)
    beyond = columns(last)

    def finish(x, fixed, flux):
        values = [pull(last, x, fixed, beyond, q) for q in range(26)]
        for q in range(26):
            result[q, x] = (KEEP_FLOW if q < 19 else KEEP_HEAT) ** STEPS * values[q]
        _, warmth, _, u = moments(values[:19], values[19:], KEEP_HEAT**STEPS)
        return flux + u[2] * warmth

    flux = jnp.zeros((ny, nz), jnp.float32)
    for x in (0, nx - 1):
        flux = finish(x, x, flux)
    flux = lax.fori_loop(1, nx - 1, lambda x, t: finish(x, None, t), flux, unroll=UNROLL)
    sums[me] = jnp.sum(flux, axis=0, keepdims=True)

    def send_sum(target):
        pltpu.make_async_remote_copy(
            src_ref=sums.at[me], dst_ref=sums.at[me],
            send_sem=sum_send, recv_sem=sum_recv, device_id=target,
        ).start()

    if joined:
        xs, ys, zs = (
            [lax.rem(at + d, n) for d in range(n)] for at, n in zip((gx, gy, gz), sizes)
        )
        for dz in reversed(range(count_z)):
            for dx in reversed(range(count_x)):
                for dy in reversed(range(count_y)):
                    if dx or dy or dz:
                        send_sum({"gx": xs[dx], "gy": ys[dy], "gz": zs[dz]})
    else:
        pl.loop(1, everyone)(lambda d: send_sum(ahead(d)))

    settle(send_sem.at[0], STEPS * rows(v for v in LINKS if v[2] == 0))
    for sign in SIDES:
        @pl.when(has[sign])
        def _():
            settle(send_sem.at[1 + side(sign)], STEPS * rows(v for v in LINKS if v[2] == sign))
    all_rows = pltpu.make_async_remote_copy(
        src_ref=sums.at[pl.ds(0, everyone - 1)], dst_ref=sums.at[pl.ds(0, everyone - 1)],
        send_sem=sum_send, recv_sem=sum_recv, device_id=ahead(1),
    )
    all_rows.wait_send()
    all_rows.wait_recv()
    result[26, 0, 0:1, :] = jnp.sum(sums[...], axis=0)


def write_out(scale, result, flow_out, heat_out, nusselt_out, small, sem):
    copies = (
        pltpu.make_async_copy(result.at[0:19], flow_out, sem.at[0]),
        pltpu.make_async_copy(result.at[19:26], heat_out, sem.at[1]),
        pltpu.make_async_copy(small, nusselt_out, sem.at[2]),
    )
    for copy in copies[:2]:
        copy.start()
    small[...] = 1.0 + scale * jnp.sum(result[26, 0, 0:1, :], axis=1, keepdims=True)
    copies[2].start()
    for copy in copies:
        copy.wait()


def per_device(sizes, flow_pops, heat_pops):
    nx, ny, nz = flow_pops.shape[1:]
    count_x, count_y, count_z = sizes
    f32 = jnp.float32
    dma = pltpu.SemaphoreType.DMA
    cells = nx * ny * nz * count_x * count_y * count_z
    scale = nz * count_z / (DIFFUSIVITY * (HOT_WALL - COLD_WALL)) / cells * KEEP_HEAT**STEPS
    hbm = pl.BlockSpec(memory_space=pltpu.HBM)
    vmem = pl.BlockSpec(memory_space=pltpu.VMEM)
    result = pl.pallas_call(
        functools.partial(kernel, sizes),
        out_shape=pltpu.VMEM((27, nx, ny, nz), f32),
        in_specs=[hbm, hbm],
        out_specs=vmem,
        scratch_shapes=[
            pltpu.VMEM((26, nx, ny, nz), f32),
            pltpu.VMEM((STEPS, 26, nx + 2, ny, nz), f32),
            pltpu.VMEM((26, nx, ny, nz), f32),
            pltpu.VMEM((STEPS, 2, FACE, nx + 2, 1, nz), f32),
            pltpu.VMEM((STEPS, 2, FACE, nx + 2, 1, nz), f32),
            pltpu.VMEM((STEPS, 2, 2, ny, nz), f32),
            pltpu.VMEM((STEPS, 2, 3, ny, nz), f32),
            pltpu.VMEM((STEPS, 2, 2, 1, nz), f32),
            pltpu.VMEM((STEPS, 2, 2, 1, nz), f32),
            pltpu.VMEM((count_x * count_y * count_z, 1, nz), f32),
            pltpu.VMEM((STEPS * 2 * (FACE * (nx + ny) + 2), 1, nz), f32),
            dma((3,)),
            dma((3,)),
            dma((STEPS, 3)),
            dma,
            dma,
        ],
        compiler_params=pltpu.CompilerParams(
            collective_id=0, has_side_effects=True, vmem_limit_bytes=55000000
        ),
    )(pltpu.with_memory_space_constraint(flow_pops, pltpu.HBM), pltpu.with_memory_space_constraint(heat_pops, pltpu.HBM))
    flow, heat, nusselt = pl.pallas_call(
        functools.partial(write_out, scale),
        out_shape=(
            jax.ShapeDtypeStruct(flow_pops.shape, f32),
            jax.ShapeDtypeStruct(heat_pops.shape, f32),
            jax.ShapeDtypeStruct((1, 1), f32),
        ),
        in_specs=[vmem],
        out_specs=(hbm, hbm, hbm),
        scratch_shapes=[pltpu.VMEM((1, 1), f32), dma((3,))],
        compiler_params=pltpu.CompilerParams(vmem_limit_bytes=1024 * 1024),
    )(result)
    return flow, heat, nusselt.reshape(())


def solution(mesh):
    placed = P(None, "gx", "gy", "gz")
    sizes = tuple(mesh.shape[a] for a in ("gx", "gy", "gz"))
    return jax.shard_map(
        functools.partial(per_device, sizes),
        mesh=mesh,
        in_specs=(placed, placed),
        out_specs=(placed, placed, P()),
        check_vma=False,
    )
```

```python
import functools

import jax
import jax.numpy as jnp
import numpy as np
from jax import lax
from jax.experimental import pallas as pl
from jax.experimental.pallas import tpu as pltpu
from jax.sharding import PartitionSpec as P

STEPS = 3

FLOW_SET = np.array(
    [
        [0, 0, 0],
        [1, 0, 0],
        [-1, 0, 0],
        [0, 1, 0],
        [0, -1, 0],
        [0, 0, 1],
        [0, 0, -1],
        [1, 1, 0],
        [-1, -1, 0],
        [1, -1, 0],
        [-1, 1, 0],
        [1, 0, 1],
        [-1, 0, -1],
        [1, 0, -1],
        [-1, 0, 1],
        [0, 1, 1],
        [0, -1, -1],
        [0, 1, -1],
        [0, -1, 1],
    ]
)
FLOW_WEIGHT = np.array([1.0 / 3.0] + [1.0 / 18.0] * 6 + [1.0 / 36.0] * 12)
HEAT_WEIGHT = np.array([0.25] + [0.125] * 6)
LATTICE = [tuple(int(c) for c in v) for v in np.concatenate([FLOW_SET, FLOW_SET[:7]], axis=0)]
WEIGHTS = [float(w) for w in np.concatenate([FLOW_WEIGHT, HEAT_WEIGHT])]
OPPOSITE = (
    [0]
    + [q + 1 if q % 2 else q - 1 for q in range(1, 19)]
    + [19]
    + [q - 1 if q % 2 else q + 1 for q in range(20, 26)]
)
TAU_FLOW = 0.6
TAU_HEAT = 0.7
GRAVITY_LIFT = 0.01
HOT_WALL = 0.5
COLD_WALL = -0.5
DIFFUSIVITY = (TAU_HEAT - 0.5) / 4.0
KEEP_FLOW = 1.0 - 1.0 / TAU_FLOW
KEEP_HEAT = 1.0 - 1.0 / TAU_HEAT

MEMBERS = {
    (axis, sign): [q for q in range(26) if LATTICE[q][axis] == sign]
    for axis in range(3)
    for sign in (1, -1)
}
FACE = len(MEMBERS[0, 1])
STORED = (
    MEMBERS[0, 1] + MEMBERS[0, -1] + [q for q in range(26) if LATTICE[q][0] == 0]
)
SLOT = [STORED.index(q) for q in range(26)]
SIDES = (1, -1)
UNROLL = True
LINKS = sorted({v for v in LATTICE if v != (0, 0, 0)})


EARLY = sorted([v for v in LINKS if v[0]], key=lambda v: sum(abs(c) for c in v))
LATE = sorted([v for v in LINKS if not v[0]], key=lambda v: -sum(abs(c) for c in v))


def group(v):
    return 0 if v[2] == 0 else 1 + side(v[2])


def side(sign):
    return 0 if sign == 1 else 1


def total(terms):
    terms = list(terms)
    while len(terms) > 1:
        terms = [a + b for a, b in zip(terms[::2], terms[1::2])] + terms[len(terms) & ~1 :]
    return terms[0]


def gather(values, span):
    flat = [values[q - span[0]] for q in span if LATTICE[q][2] == 0]
    tilted = [values[q - span[0]] for q in span if LATTICE[q][2]]
    return total(flat) + total(tilted)


def moments(f, g, scale):
    rho, warmth = gather(f, range(19)), gather(g, range(19, 26))
    flow = []
    for axis in range(3):
        result = None
        for q in sorted(range(1, 19, 2), key=lambda q: abs(LATTICE[q][2])):
            if LATTICE[q][axis]:
                odd = f[q] - f[q + 1]
                if result is None:
                    result = odd
                else:
                    result = result + odd if LATTICE[q][axis] == 1 else result - odd
        flow.append(result)
    half = (0.5 * GRAVITY_LIFT * scale) * warmth
    inv = 1.0 / rho
    return rho, warmth, half, (flow[0] * inv, flow[1] * inv, flow[2] * inv + half)


def collide(f, g, scale):
    rho, warmth, half, u = moments(f, g, scale)
    push = rho * half
    rate = 1.0 / TAU_FLOW
    lift = 2.0 * (1.0 - 0.5 / TAU_FLOW)
    weight = WEIGHTS[7] / KEEP_FLOW
    square = u[0] * u[0] + u[1] * u[1] + u[2] * u[2]
    base = (weight * rate * rho) * (1.0 - 1.5 * square) - (3.0 * lift * weight) * (u[2] * push)
    quad = (4.5 * rate * weight) * rho
    line = (3.0 * rate * weight) * rho
    push3 = (3.0 * lift * weight) * push
    push9 = (9.0 * lift * weight) * push
    small = (base, quad, line, push3, push9)
    large = tuple((WEIGHTS[1] / WEIGHTS[7]) * part for part in small)
    post = [None] * 26
    post[0] = f[0] + (WEIGHTS[0] / WEIGHTS[7]) * base
    for q in range(1, 19, 2):
        c = LATTICE[q]
        along = None
        for axis in range(3):
            if c[axis]:
                if along is None:
                    along = u[axis]
                else:
                    along = along + u[axis] if c[axis] == 1 else along - u[axis]
        base, quad, line, push3, push9 = large if q < 7 else small
        inner = quad * along
        odd = line * along
        if c[2] == 1:
            inner, odd = inner + push9, odd + push3
        elif c[2] == -1:
            inner, odd = inner - push9, odd - push3
        even = base + along * inner
        post[q] = f[q] + (even + odd)
        post[q + 1] = f[q + 1] + (even - odd)
    share = 1.0 / (TAU_HEAT * KEEP_HEAT)
    post[19] = g[0] + (WEIGHTS[19] * share) * warmth
    still = (WEIGHTS[20] * share) * warmth
    slope = (4.0 * WEIGHTS[20] * share) * warmth
    for axis in range(3):
        drift = slope * u[axis]
        q = 20 + 2 * axis
        post[q] = g[q - 19] + (still + drift)
        post[q + 1] = g[q - 18] + (still - drift)
    return post


def kernel(
    sizes, flow_in, heat_in, result,
    cur, post, mid, sy, ry, sz, rz, sxz, rxz, syz, ryz, sums, ledger,
    in_sem, send_sem, recv_sem, sum_send, sum_recv,
):
    count_x, count_y, count_z = sizes
    nx, ny, nz = cur.shape[1:]
    gx, gy, gz = (lax.axis_index(a) for a in ("gx", "gy", "gz"))
    has = {1: gz < count_z - 1, -1: gz > 0}
    everyone = count_x * count_y * count_z
    me = (gx * count_y + gy) * count_z + gz

    def device(v):
        return {
            "gx": lax.rem(gx + v[0] + count_x, count_x),
            "gy": lax.rem(gy + v[1] + count_y, count_y),
            "gz": gz + v[2],
        }

    def ahead(distance):
        other = lax.rem(me + distance, everyone)
        row = other // count_z
        return {"gx": row // count_y, "gy": lax.rem(row, count_y), "gz": lax.rem(other, count_z)}

    def load(part, x):
        return (
            pltpu.make_async_copy(flow_in.at[:, x], cur.at[0:19, x], in_sem.at[part]),
            pltpu.make_async_copy(heat_in.at[:, x], cur.at[19:26, x], in_sem.at[part]),
        )

    loads = [load(0, 0), load(1, nx - 1), [c for x in range(1, nx - 1) for c in load(2, x)]]
    for copies in loads:
        for copy in copies:
            copy.start()

    barrier = pltpu.get_barrier_semaphore()
    near = sorted({(v[0] % count_x, v[1] % count_y, v[2]) for v in LINKS})
    reach = (count_x // 2, count_y // 2, count_z - 1)
    joined = max(reach) <= STEPS and sum(reach) <= 2 * STEPS
    if joined:
        for v in near:
            if v[2] == 0:
                pl.semaphore_signal(barrier, inc=1, device_id=device(v))
        for sign in SIDES:
            @pl.when(has[sign])
            def _():
                for v in near:
                    if v[2] == sign:
                        pl.semaphore_signal(barrier, inc=1, device_id=device(v))
    else:
        @pl.loop(1, everyone)
        def _(d):
            pl.semaphore_signal(barrier, inc=1, device_id=ahead(d))

    def greet():
        if joined:
            count = len([v for v in near if v[2] == 0])
            for sign in SIDES:
                count += jnp.where(has[sign], len([v for v in near if v[2] == sign]), 0)
        else:
            count = everyone - 1
        pl.semaphore_wait(barrier, count)

    lane = lax.broadcasted_iota(jnp.int32, (ny, nz), 1)
    row = lax.broadcasted_iota(jnp.int32, (ny, nz), 0)
    first_row, last_row = row == 0, row == ny - 1
    first_lane, last_lane = lane == 0, lane == nz - 1
    place = lax.rem(lane, FACE)
    slant = {1: lane == lax.rem(nz - row, nz), -1: lane == nz - 1 - row}

    def lanes_of(sign, pick):
        mask = None
        for j, q in enumerate(MEMBERS[2, sign]):
            if pick(q):
                mask = place == j if mask is None else mask | (place == j)
        return mask

    def message(s, v):
        x, y, z = v
        if z == 0:
            start = 0 if x == 1 else FACE
            edge, halo = (nx, 0) if x == 1 else (1, nx + 1)
            if y == 0:
                src = post.at[s, start : start + FACE, edge]
                dst = post.at[s, start : start + FACE, halo]
            elif x == 0:
                src = sy.at[s, side(y), :, 1 : nx + 1]
                dst = ry.at[s, side(y), :, 1 : nx + 1]
            else:
                j = MEMBERS[1, y].index(LATTICE.index(v))
                src = sy.at[s, side(y), j, edge]
                dst = ry.at[s, side(y), j, halo]
        elif y == 0:
            src = sz.at[s, side(z)] if x == 0 else sxz.at[s, side(z), side(x)]
            dst = rz.at[s, side(z)] if x == 0 else rxz.at[s, side(z), side(x)]
        else:
            src = syz.at[s, side(z), side(y)]
            dst = ryz.at[s, side(z), side(y)]
        return pltpu.make_async_remote_copy(
            src_ref=src, dst_ref=dst, send_sem=send_sem.at[group(v)], recv_sem=recv_sem.at[s, group(v)],
            device_id=device(v),
        )

    def send(s, links):
        for v in links:
            if v[2] == 0:
                message(s, v).start()
        for sign in SIDES:
            if any(v[2] == sign for v in links):
                @pl.when(has[sign])
                def _():
                    for v in links:
                        if v[2] == sign:
                            message(s, v).start()

    def rows(links):
        count = 0
        for x, y, z in links:
            if y == 0:
                count += FACE * ny if z == 0 else ny if x == 0 else 1
            else:
                count += FACE * nx if x == 0 and z == 0 else 1
        return count

    def settle(sem, count):
        pltpu.make_async_copy(ledger.at[0:count], ledger.at[0:count], sem).wait()

    def receive(s):
        settle(recv_sem.at[s, 0], rows(v for v in LINKS if v[2] == 0))
        for sign in SIDES:
            @pl.when(has[-sign])
            def _():
                settle(recv_sem.at[s, 1 + side(sign)], rows(v for v in LINKS if v[2] == sign))

    def flatten(sign, tile, at):
        column = jnp.broadcast_to(tile[:, at : at + 1], (ny, nz))
        return jnp.sum(jnp.where(slant[sign], column, 0.0), axis=0, keepdims=True)

    def target(x, q):
        return lax.rem(x + (LATTICE[q][0] + nx), nx) * FACE

    def keep_plane(s, x, values, packs):
        for q in range(26):
            post[s, SLOT[q], x + 1] = values[q]
        for sign in SIDES:
            r = ny - 1 if sign == 1 else 0
            for j, q in enumerate(MEMBERS[1, sign]):
                value = values[q]
                if LATTICE[q][2]:
                    value = pltpu.roll(value, LATTICE[q][2] % nz, 1)
                sy[s, side(sign), j, x + 1] = value[r : r + 1, :]
        new = []
        for sign, pack in zip(SIDES, packs):
            source = nz - 1 if sign == 1 else 0
            for j, q in enumerate(MEMBERS[2, sign]):
                k = target(x, q) + j
                turned = pltpu.roll(values[q], lax.rem(k + (nz - source), nz), 1)
                pack = jnp.where(lane == k, turned, pack)
            new.append(pack)
        return tuple(new)

    def stream(s, x):
        for q in range(26):
            cx, cy, cz = LATTICE[q]
            if cy or cz:
                value = post[s, SLOT[q], x + 1]
                if cz:
                    value = pltpu.roll(value, cz % nz, 1)
                if cy:
                    value = pltpu.roll(value, cy % ny, 0)
                mid[SLOT[q], x] = value

    def bounce(s, sign, pack, unit):
        own = MEMBERS[2, sign]
        edge = (nx - 1) * FACE
        wall = pack
        for x in SIDES:
            near_part = pltpu.roll(pack, (-x * FACE) % nz, 1)
            far_part = pltpu.roll(pack, (x * edge) % nz, 1)
            far = lane >= edge if x == 1 else lane < FACE
            wall = jnp.where(
                lanes_of(sign, lambda q: LATTICE[q][0] == x), jnp.where(far, far_part, near_part), wall
            )
        for y in SIDES:
            wall = jnp.where(
                lanes_of(sign, lambda q: LATTICE[q][1] == y), pltpu.roll(pack, -y % ny, 0), wall
            )
        weight = WEIGHTS[own[-1]]
        warm = (2.0 * weight * (COLD_WALL if sign == 1 else HOT_WALL)) * unit
        wall = jnp.where(lanes_of(sign, lambda q: q >= 19), warm - wall, wall)
        rz[s, side(-sign)] = wall
        for x in SIDES:
            q = LATTICE.index((x, 0, -sign))
            at = (0 if x == 1 else nx - 1) * FACE + MEMBERS[2, -sign].index(q)
            rxz[s, side(-sign), side(x)] = flatten(-sign, wall, at)

    def arrive():
        planes = ((0, cur.at[:, 0]), (1, cur.at[:, nx - 1]), (2, cur.at[:, 1 : nx - 1]))
        for part, planes_of in planes:
            pltpu.make_async_copy(planes_of, planes_of, in_sem.at[part]).wait()
            if part:
                yield

    def advance(s, body, arrive, before_send, unit):
        zero = jnp.zeros((ny, nz), jnp.float32)
        packs = (zero, zero)
        stages = iter(arrive() or ())
        next(stages, None)
        for x in (0, nx - 1):
            values = body(x, x)
            packs = keep_plane(s, x, values, packs)
            for sign in SIDES:
                v = (1 if x else -1, 0, sign)
                sxz[s, side(sign), side(v[0])] = flatten(sign, values[LATTICE.index(v)], nz - 1 if sign == 1 else 0)
        before_send()
        send(s, [v for v in EARLY if v[1] and not v[2]])
        send(s, [v for v in EARLY if not v[1] and not v[2]])
        send(s, [v for v in EARLY if v[2]])
        next(stages, None)
        packs = lax.fori_loop(
            1, nx - 1, lambda x, p: keep_plane(s, x, body(x, None), p), packs, unroll=UNROLL
        )
        send(s, [v for v in LATE if v[2] == 0])
        for sign, pack in zip(SIDES, packs):
            whole = pack
            for y in SIDES:
                whole = jnp.where(
                    lanes_of(sign, lambda q: LATTICE[q][1] == y), pltpu.roll(pack, y % ny, 0), whole
                )
            sz[s, side(sign)] = whole
            for y in SIDES:
                r = 0 if y == 1 else ny - 1
                syz[s, side(sign), side(y)] = whole[r : r + 1, :]
        send(s, [v for v in LATE if v[2]])
        for sign in SIDES:
            @pl.when(jnp.logical_not(has[sign]))
            def _():
                bounce(s, sign, sz[s, side(sign)], unit)
        lax.fori_loop(0, nx, lambda x, c: (stream(s, x), c)[1], 0, unroll=2)

    def columns(s):
        result = {}
        for sign in SIDES:
            tile = rz[s, side(sign)]
            for y in SIDES:
                mask = lanes_of(sign, lambda q: LATTICE[q][1] == y) & (first_row if y == 1 else last_row)
                edge = jnp.broadcast_to(ryz[s, side(sign), side(y)], (ny, nz))
                tile = jnp.where(mask & has[-sign], edge, tile)
            result[sign] = tile
        return result

    def pull(s, x, fixed, beyond, q):
        cx, cy, cz = LATTICE[q]
        at = x - cx + 1
        if fixed is not None and fixed - cx in (-1, nx):
            value = post[s, SLOT[q], at]
            if cz:
                value = pltpu.roll(value, cz % nz, 1)
            if cy:
                value = pltpu.roll(value, cy % ny, 0)
        elif cy or cz:
            value = mid[SLOT[q], at - 1]
        else:
            value = post[s, SLOT[q], at]
        if cy:
            j = MEMBERS[1, cy].index(q)
            edge = jnp.broadcast_to(ry[s, side(cy), j, at], (ny, nz))
            value = jnp.where(first_row if cy == 1 else last_row, edge, value)
        if cz:
            j = MEMBERS[2, cz].index(q)
            end = 0 if cz == 1 else nz - 1
            if fixed is not None and fixed - cx in (-1, nx):
                line = jnp.broadcast_to(rxz[s, side(cz), side(cx)], (ny, nz))
                outer = pltpu.roll(line, 0, 1, stride=1, stride_axis=0)
            else:
                outer = pltpu.roll(beyond[cz], lax.rem(end + nz - (x * FACE + j), nz), 1)
            value = jnp.where(first_lane if cz == 1 else last_lane, outer, value)
        return value

    def fresh(x, fixed):
        return collide([cur[q, x] for q in range(19)], [cur[q, x] for q in range(19, 26)], 1.0)

    advance(0, fresh, arrive, greet, 1.0 / KEEP_HEAT)

    def step(s, carry):
        scale, unit = carry
        receive(s)
        beyond = columns(s)

        def body(x, fixed):
            values = [pull(s, x, fixed, beyond, q) for q in range(26)]
            return collide(values[:19], values[19:], scale)

        unit = unit * (1.0 / KEEP_HEAT)
        advance(s + 1, body, lambda: None, lambda: None, unit)
        return scale * KEEP_HEAT, unit

    lax.fori_loop(0, STEPS - 1, step, (jnp.float32(KEEP_HEAT), jnp.float32(1.0 / KEEP_HEAT)))

    last = STEPS - 1
    receive(last)
    beyond = columns(last)

    def finish(x, fixed, flux):
        values = [pull(last, x, fixed, beyond, q) for q in range(26)]
        for q in range(26):
            result[q, x] = (KEEP_FLOW if q < 19 else KEEP_HEAT) ** STEPS * values[q]
        _, warmth, _, u = moments(values[:19], values[19:], KEEP_HEAT**STEPS)
        return flux + u[2] * warmth

    flux = jnp.zeros((ny, nz), jnp.float32)
    for x in (0, nx - 1):
        flux = finish(x, x, flux)
    flux = lax.fori_loop(1, nx - 1, lambda x, t: finish(x, None, t), flux, unroll=UNROLL)
    sums[me] = jnp.sum(flux, axis=0, keepdims=True)

    def send_sum(target):
        pltpu.make_async_remote_copy(
            src_ref=sums.at[me], dst_ref=sums.at[me],
            send_sem=sum_send, recv_sem=sum_recv, device_id=target,
        ).start()

    if joined:
        xs, ys, zs = (
            [lax.rem(at + d, n) for d in range(n)] for at, n in zip((gx, gy, gz), sizes)
        )
        for dz in reversed(range(count_z)):
            for dx in reversed(range(count_x)):
                for dy in reversed(range(count_y)):
                    if dx or dy or dz:
                        send_sum({"gx": xs[dx], "gy": ys[dy], "gz": zs[dz]})
    else:
        pl.loop(1, everyone)(lambda d: send_sum(ahead(d)))

    settle(send_sem.at[0], STEPS * rows(v for v in LINKS if v[2] == 0))
    for sign in SIDES:
        @pl.when(has[sign])
        def _():
            settle(send_sem.at[1 + side(sign)], STEPS * rows(v for v in LINKS if v[2] == sign))
    all_rows = pltpu.make_async_remote_copy(
        src_ref=sums.at[pl.ds(0, everyone - 1)], dst_ref=sums.at[pl.ds(0, everyone - 1)],
        send_sem=sum_send, recv_sem=sum_recv, device_id=ahead(1),
    )
    all_rows.wait_send()
    all_rows.wait_recv()
    result[26, 0, 0:1, :] = jnp.sum(sums[...], axis=0)


def write_out(scale, result, flow_out, heat_out, nusselt_out, small, sem):
    copies = (
        pltpu.make_async_copy(result.at[0:19], flow_out, sem.at[0]),
        pltpu.make_async_copy(result.at[19:26], heat_out, sem.at[1]),
        pltpu.make_async_copy(small, nusselt_out, sem.at[2]),
    )
    for copy in copies[:2]:
        copy.start()
    small[...] = 1.0 + scale * jnp.sum(result[26, 0, 0:1, :], axis=1, keepdims=True)
    copies[2].start()
    for copy in copies:
        copy.wait()


def per_device(sizes, flow_pops, heat_pops):
    nx, ny, nz = flow_pops.shape[1:]
    count_x, count_y, count_z = sizes
    f32 = jnp.float32
    dma = pltpu.SemaphoreType.DMA
    cells = nx * ny * nz * count_x * count_y * count_z
    scale = nz * count_z / (DIFFUSIVITY * (HOT_WALL - COLD_WALL)) / cells * KEEP_HEAT**STEPS
    hbm = pl.BlockSpec(memory_space=pltpu.HBM)
    vmem = pl.BlockSpec(memory_space=pltpu.VMEM)
    result = pl.pallas_call(
        functools.partial(kernel, sizes),
        out_shape=pltpu.VMEM((27, nx, ny, nz), f32),
        in_specs=[hbm, hbm],
        out_specs=vmem,
        scratch_shapes=[
            pltpu.VMEM((26, nx, ny, nz), f32),
            pltpu.VMEM((STEPS, 26, nx + 2, ny, nz), f32),
            pltpu.VMEM((26, nx, ny, nz), f32),
            pltpu.VMEM((STEPS, 2, FACE, nx + 2, 1, nz), f32),
            pltpu.VMEM((STEPS, 2, FACE, nx + 2, 1, nz), f32),
            pltpu.VMEM((STEPS, 2, ny, nz), f32),
            pltpu.VMEM((STEPS, 2, ny, nz), f32),
            pltpu.VMEM((STEPS, 2, 2, 1, nz), f32),
            pltpu.VMEM((STEPS, 2, 2, 1, nz), f32),
            pltpu.VMEM((STEPS, 2, 2, 1, nz), f32),
            pltpu.VMEM((STEPS, 2, 2, 1, nz), f32),
            pltpu.VMEM((count_x * count_y * count_z, 1, nz), f32),
            pltpu.VMEM((STEPS * 2 * (FACE * (nx + ny) + 2), 1, nz), f32),
            dma((3,)),
            dma((3,)),
            dma((STEPS, 3)),
            dma,
            dma,
        ],
        compiler_params=pltpu.CompilerParams(
            collective_id=0, has_side_effects=True, vmem_limit_bytes=55000000
        ),
    )(pltpu.with_memory_space_constraint(flow_pops, pltpu.HBM), pltpu.with_memory_space_constraint(heat_pops, pltpu.HBM))
    flow, heat, nusselt = pl.pallas_call(
        functools.partial(write_out, scale),
        out_shape=(
            jax.ShapeDtypeStruct(flow_pops.shape, f32),
            jax.ShapeDtypeStruct(heat_pops.shape, f32),
            jax.ShapeDtypeStruct((1, 1), f32),
        ),
        in_specs=[vmem],
        out_specs=(hbm, hbm, hbm),
        scratch_shapes=[pltpu.VMEM((1, 1), f32), dma((3,))],
        compiler_params=pltpu.CompilerParams(vmem_limit_bytes=1024 * 1024),
    )(result)
    return flow, heat, nusselt.reshape(())


def solution(mesh):
    placed = P(None, "gx", "gy", "gz")
    sizes = tuple(mesh.shape[a] for a in ("gx", "gy", "gz"))
    return jax.shard_map(
        functools.partial(per_device, sizes),
        mesh=mesh,
        in_specs=(placed, placed),
        out_specs=(placed, placed, P()),
        check_vma=False,
    )
```

```python
import functools

import jax
import jax.numpy as jnp
import numpy as np
from jax import lax
from jax.experimental import pallas as pl
from jax.experimental.pallas import tpu as pltpu
from jax.sharding import PartitionSpec as P

STEPS = 3

FLOW_SET = np.array(
    [
        [0, 0, 0],
        [1, 0, 0],
        [-1, 0, 0],
        [0, 1, 0],
        [0, -1, 0],
        [0, 0, 1],
        [0, 0, -1],
        [1, 1, 0],
        [-1, -1, 0],
        [1, -1, 0],
        [-1, 1, 0],
        [1, 0, 1],
        [-1, 0, -1],
        [1, 0, -1],
        [-1, 0, 1],
        [0, 1, 1],
        [0, -1, -1],
        [0, 1, -1],
        [0, -1, 1],
    ]
)
FLOW_WEIGHT = np.array([1.0 / 3.0] + [1.0 / 18.0] * 6 + [1.0 / 36.0] * 12)
HEAT_WEIGHT = np.array([0.25] + [0.125] * 6)
LATTICE = [tuple(int(c) for c in v) for v in np.concatenate([FLOW_SET, FLOW_SET[:7]], axis=0)]
WEIGHTS = [float(w) for w in np.concatenate([FLOW_WEIGHT, HEAT_WEIGHT])]
OPPOSITE = (
    [0]
    + [q + 1 if q % 2 else q - 1 for q in range(1, 19)]
    + [19]
    + [q - 1 if q % 2 else q + 1 for q in range(20, 26)]
)
TAU_FLOW = 0.6
TAU_HEAT = 0.7
GRAVITY_LIFT = 0.01
HOT_WALL = 0.5
COLD_WALL = -0.5
DIFFUSIVITY = (TAU_HEAT - 0.5) / 4.0
KEEP_FLOW = 1.0 - 1.0 / TAU_FLOW
KEEP_HEAT = 1.0 - 1.0 / TAU_HEAT

MEMBERS = {
    (axis, sign): [q for q in range(26) if LATTICE[q][axis] == sign]
    for axis in range(3)
    for sign in (1, -1)
}
FACE = len(MEMBERS[0, 1])
STORED = (
    MEMBERS[0, 1] + MEMBERS[0, -1] + [q for q in range(26) if LATTICE[q][0] == 0]
)
SLOT = [STORED.index(q) for q in range(26)]
SIDES = (1, -1)
UNROLL = True
LINKS = sorted({v for v in LATTICE if v != (0, 0, 0)})


EARLY = sorted([v for v in LINKS if v[0]], key=lambda v: sum(abs(c) for c in v))
LATE = sorted([v for v in LINKS if not v[0]], key=lambda v: -sum(abs(c) for c in v))


def group(v):
    return 0 if v[2] == 0 else 1 + side(v[2])


def side(sign):
    return 0 if sign == 1 else 1


def total(terms):
    terms = list(terms)
    while len(terms) > 1:
        terms = [a + b for a, b in zip(terms[::2], terms[1::2])] + terms[len(terms) & ~1 :]
    return terms[0]


def gather(values, span):
    flat = [values[q - span[0]] for q in span if LATTICE[q][2] == 0]
    tilted = [values[q - span[0]] for q in span if LATTICE[q][2]]
    return total(flat) + total(tilted)


def moments(f, g, scale):
    rho, warmth = gather(f, range(19)), gather(g, range(19, 26))
    flow = []
    for axis in range(3):
        result = None
        for q in sorted(range(1, 19, 2), key=lambda q: abs(LATTICE[q][2])):
            if LATTICE[q][axis]:
                odd = f[q] - f[q + 1]
                if result is None:
                    result = odd
                else:
                    result = result + odd if LATTICE[q][axis] == 1 else result - odd
        flow.append(result)
    half = (0.5 * GRAVITY_LIFT * scale) * warmth
    inv = 1.0 / rho
    return rho, warmth, half, (flow[0] * inv, flow[1] * inv, flow[2] * inv + half)


def collide(f, g, scale):
    rho, warmth, half, u = moments(f, g, scale)
    push = rho * half
    rate = 1.0 / TAU_FLOW
    lift = 2.0 * (1.0 - 0.5 / TAU_FLOW)
    weight = WEIGHTS[7] / KEEP_FLOW
    square = u[0] * u[0] + u[1] * u[1] + u[2] * u[2]
    base = (weight * rate * rho) * (1.0 - 1.5 * square) - (3.0 * lift * weight) * (u[2] * push)
    quad = (4.5 * rate * weight) * rho
    line = (3.0 * rate * weight) * rho
    push3 = (3.0 * lift * weight) * push
    push9 = (9.0 * lift * weight) * push
    small = (base, quad, line, push3, push9)
    large = tuple((WEIGHTS[1] / WEIGHTS[7]) * part for part in small)
    post = [None] * 26
    post[0] = f[0] + (WEIGHTS[0] / WEIGHTS[7]) * base
    for q in range(1, 19, 2):
        c = LATTICE[q]
        along = None
        for axis in range(3):
            if c[axis]:
                if along is None:
                    along = u[axis]
                else:
                    along = along + u[axis] if c[axis] == 1 else along - u[axis]
        base, quad, line, push3, push9 = large if q < 7 else small
        inner = quad * along
        odd = line * along
        if c[2] == 1:
            inner, odd = inner + push9, odd + push3
        elif c[2] == -1:
            inner, odd = inner - push9, odd - push3
        even = base + along * inner
        post[q] = f[q] + (even + odd)
        post[q + 1] = f[q + 1] + (even - odd)
    share = 1.0 / (TAU_HEAT * KEEP_HEAT)
    post[19] = g[0] + (WEIGHTS[19] * share) * warmth
    still = (WEIGHTS[20] * share) * warmth
    slope = (4.0 * WEIGHTS[20] * share) * warmth
    for axis in range(3):
        drift = slope * u[axis]
        q = 20 + 2 * axis
        post[q] = g[q - 19] + (still + drift)
        post[q + 1] = g[q - 18] + (still - drift)
    return post


def kernel(
    sizes, flow_in, heat_in, result,
    cur, post, mid, sy, ry, sz, rz, sxz, rxz, syz, ryz, sums, ledger,
    in_sem, send_sem, recv_sem, sum_send, sum_recv,
):
    count_x, count_y, count_z = sizes
    nx, ny, nz = cur.shape[1:]
    gx, gy, gz = (lax.axis_index(a) for a in ("gx", "gy", "gz"))
    has = {1: gz < count_z - 1, -1: gz > 0}
    everyone = count_x * count_y * count_z
    me = (gx * count_y + gy) * count_z + gz

    def device(v):
        return {
            "gx": lax.rem(gx + v[0] + count_x, count_x),
            "gy": lax.rem(gy + v[1] + count_y, count_y),
            "gz": gz + v[2],
        }

    def ahead(distance):
        other = lax.rem(me + distance, everyone)
        row = other // count_z
        return {"gx": row // count_y, "gy": lax.rem(row, count_y), "gz": lax.rem(other, count_z)}

    def load(part, x):
        return (
            pltpu.make_async_copy(flow_in.at[:, x], cur.at[0:19, x], in_sem.at[part]),
            pltpu.make_async_copy(heat_in.at[:, x], cur.at[19:26, x], in_sem.at[part]),
        )

    def pieces(part, x):
        cuts = (0, 7, 13, 19)
        return [
            pltpu.make_async_copy(flow_in.at[a:b, x], cur.at[a:b, x], in_sem.at[part])
            for a, b in zip(cuts, cuts[1:])
        ] + [pltpu.make_async_copy(heat_in.at[:, x], cur.at[19:26, x], in_sem.at[part])]

    loads = [pieces(0, 0), pieces(1, nx - 1), [c for x in range(1, nx - 1) for c in load(2, x)]]
    def fetch(parts):
        for copies in parts:
            for copy in copies:
                copy.start()

    fetch(loads[:2])
    barrier = pltpu.get_barrier_semaphore()
    near = sorted(
        {(v[0] % count_x, v[1] % count_y, v[2]) for v in LINKS}, key=lambda v: -sum(c != 0 for c in v)
    )
    reach = (count_x // 2, count_y // 2, count_z - 1)
    joined = max(reach) <= STEPS and sum(reach) <= 2 * STEPS
    if joined:
        for sign in SIDES:
            @pl.when(has[sign])
            def _():
                for v in near:
                    if v[2] == sign:
                        pl.semaphore_signal(barrier, inc=1, device_id=device(v))
        for v in near:
            if v[2] == 0:
                pl.semaphore_signal(barrier, inc=1, device_id=device(v))
    else:
        @pl.loop(1, everyone)
        def _(d):
            pl.semaphore_signal(barrier, inc=1, device_id=ahead(d))
    fetch(loads[2:])

    def greet():
        if joined:
            count = len([v for v in near if v[2] == 0])
            for sign in SIDES:
                count += jnp.where(has[sign], len([v for v in near if v[2] == sign]), 0)
        else:
            count = everyone - 1
        pl.semaphore_wait(barrier, count)

    lane = lax.broadcasted_iota(jnp.int32, (ny, nz), 1)
    row = lax.broadcasted_iota(jnp.int32, (ny, nz), 0)
    first_row, last_row = row == 0, row == ny - 1
    first_lane, last_lane = lane == 0, lane == nz - 1
    place = lax.rem(lane, FACE)
    slant = {1: lane == lax.rem(nz - row, nz), -1: lane == nz - 1 - row}

    def lanes_of(sign, pick):
        mask = None
        for j, q in enumerate(MEMBERS[2, sign]):
            if pick(q):
                mask = place == j if mask is None else mask | (place == j)
        return mask

    def message(s, v):
        x, y, z = v
        if z == 0:
            start = 0 if x == 1 else FACE
            edge, halo = (nx, 0) if x == 1 else (1, nx + 1)
            if y == 0:
                src = post.at[s, start : start + FACE, edge]
                dst = post.at[s, start : start + FACE, halo]
            elif x == 0:
                src = sy.at[s, side(y), :, 1 : nx + 1]
                dst = ry.at[s, side(y), :, 1 : nx + 1]
            else:
                j = MEMBERS[1, y].index(LATTICE.index(v))
                src = sy.at[s, side(y), j, edge]
                dst = ry.at[s, side(y), j, halo]
        elif y == 0:
            src = sz.at[s, side(z)] if x == 0 else sxz.at[s, side(z), side(x)]
            dst = rz.at[s, side(z)] if x == 0 else rxz.at[s, side(z), side(x)]
        else:
            src = syz.at[s, side(z), side(y)]
            dst = ryz.at[s, side(z), side(y)]
        return pltpu.make_async_remote_copy(
            src_ref=src, dst_ref=dst, send_sem=send_sem.at[group(v)], recv_sem=recv_sem.at[s, group(v)],
            device_id=device(v),
        )

    def send(s, links):
        for v in links:
            if v[2] == 0:
                message(s, v).start()
        for sign in SIDES:
            if any(v[2] == sign for v in links):
                @pl.when(has[sign])
                def _():
                    for v in links:
                        if v[2] == sign:
                            message(s, v).start()

    def rows(links):
        count = 0
        for x, y, z in links:
            if y == 0:
                count += FACE * ny if z == 0 else ny if x == 0 else 1
            else:
                count += FACE * nx if x == 0 and z == 0 else 1
        return count

    def settle(sem, count):
        pltpu.make_async_copy(ledger.at[0:count], ledger.at[0:count], sem).wait()

    def receive(s):
        settle(recv_sem.at[s, 0], rows(v for v in LINKS if v[2] == 0))
        for sign in SIDES:
            @pl.when(has[-sign])
            def _():
                settle(recv_sem.at[s, 1 + side(sign)], rows(v for v in LINKS if v[2] == sign))

    def flatten(sign, tile, at):
        column = jnp.broadcast_to(tile[:, at : at + 1], (ny, nz))
        return jnp.sum(jnp.where(slant[sign], column, 0.0), axis=0, keepdims=True)

    def target(x, q):
        return lax.rem(x + (LATTICE[q][0] + nx), nx) * FACE

    def keep_urgent(s, x, way, values):
        for q in MEMBERS[0, way]:
            post[s, SLOT[q], x + 1] = values[q]
        for y in SIDES:
            q = LATTICE.index((way, y, 0))
            r = ny - 1 if y == 1 else 0
            sy[s, side(y), MEMBERS[1, y].index(q), x + 1] = values[q][r : r + 1, :]

    def keep_plane(s, x, way, values, packs):
        for q in range(26):
            if LATTICE[q][0] != way:
                post[s, SLOT[q], x + 1] = values[q]
        for sign in SIDES:
            r = ny - 1 if sign == 1 else 0
            for j, q in enumerate(MEMBERS[1, sign]):
                if LATTICE[q][0] == way:
                    continue
                value = values[q]
                if LATTICE[q][2]:
                    value = pltpu.roll(value, LATTICE[q][2] % nz, 1)
                sy[s, side(sign), j, x + 1] = value[r : r + 1, :]
        new = []
        for sign, pack in zip(SIDES, packs):
            source = nz - 1 if sign == 1 else 0
            for j, q in enumerate(MEMBERS[2, sign]):
                k = target(x, q) + j
                turned = pltpu.roll(values[q], lax.rem(k + (nz - source), nz), 1)
                pack = jnp.where(lane == k, turned, pack)
            new.append(pack)
        return tuple(new)

    def stream(s, x):
        for q in range(26):
            cx, cy, cz = LATTICE[q]
            if cy or cz:
                value = post[s, SLOT[q], x + 1]
                if cz:
                    value = pltpu.roll(value, cz % nz, 1)
                if cy:
                    value = pltpu.roll(value, cy % ny, 0)
                mid[SLOT[q], x] = value

    def bounce(s, sign, pack, unit):
        own = MEMBERS[2, sign]
        edge = (nx - 1) * FACE
        wall = pack
        for x in SIDES:
            near_part = pltpu.roll(pack, (-x * FACE) % nz, 1)
            far_part = pltpu.roll(pack, (x * edge) % nz, 1)
            far = lane >= edge if x == 1 else lane < FACE
            wall = jnp.where(
                lanes_of(sign, lambda q: LATTICE[q][0] == x), jnp.where(far, far_part, near_part), wall
            )
        for y in SIDES:
            wall = jnp.where(
                lanes_of(sign, lambda q: LATTICE[q][1] == y), pltpu.roll(pack, -y % ny, 0), wall
            )
        weight = WEIGHTS[own[-1]]
        warm = (2.0 * weight * (COLD_WALL if sign == 1 else HOT_WALL)) * unit
        wall = jnp.where(lanes_of(sign, lambda q: q >= 19), warm - wall, wall)
        rz[s, side(-sign)] = wall
        for x in SIDES:
            q = LATTICE.index((x, 0, -sign))
            at = (0 if x == 1 else nx - 1) * FACE + MEMBERS[2, -sign].index(q)
            rxz[s, side(-sign), side(x)] = flatten(-sign, wall, at)

    def arrive():
        planes = ((0, cur.at[:, 0]), (1, cur.at[:, nx - 1]), (2, cur.at[:, 1 : nx - 1]))
        for part, planes_of in planes:
            pltpu.make_async_copy(planes_of, planes_of, in_sem.at[part]).wait()
            if part:
                yield

    def advance(s, body, arrive, before_send, unit):
        zero = jnp.zeros((ny, nz), jnp.float32)
        packs = (zero, zero)
        stages = iter(arrive() or ())
        next(stages, None)
        first = []
        for x, way in ((0, -1), (nx - 1, 1)):
            values = body(x, x)
            first.append((x, way, values))
            keep_urgent(s, x, way, values)
        before_send()
        send(s, [v for v in EARLY if v[1]])
        send(s, [v for v in EARLY if not v[1] and not v[2]])
        for x, way, values in first:
            for sign in SIDES:
                value = values[LATTICE.index((way, 0, sign))]
                sxz[s, side(sign), side(way)] = flatten(sign, value, nz - 1 if sign == 1 else 0)
        send(s, [v for v in EARLY if v[2]])
        for x, way, values in first:
            packs = keep_plane(s, x, way, values, packs)
        next(stages, None)
        packs = lax.fori_loop(
            1, nx - 1, lambda x, p: keep_plane(s, x, None, body(x, None), p), packs, unroll=UNROLL
        )
        send(s, [v for v in LATE if v[2] == 0])
        for sign, pack in zip(SIDES, packs):
            whole = pack
            for y in SIDES:
                whole = jnp.where(
                    lanes_of(sign, lambda q: LATTICE[q][1] == y), pltpu.roll(pack, y % ny, 0), whole
                )
            sz[s, side(sign)] = whole
            for y in SIDES:
                r = 0 if y == 1 else ny - 1
                syz[s, side(sign), side(y)] = whole[r : r + 1, :]
        send(s, [v for v in LATE if v[2]])
        for sign in SIDES:
            @pl.when(jnp.logical_not(has[sign]))
            def _():
                bounce(s, sign, sz[s, side(sign)], unit)
        lax.fori_loop(0, nx, lambda x, c: (stream(s, x), c)[1], 0, unroll=2)

    def columns(s):
        result = {}
        for sign in SIDES:
            tile = rz[s, side(sign)]
            for y in SIDES:
                mask = lanes_of(sign, lambda q: LATTICE[q][1] == y) & (first_row if y == 1 else last_row)
                edge = jnp.broadcast_to(ryz[s, side(sign), side(y)], (ny, nz))
                tile = jnp.where(mask & has[-sign], edge, tile)
            result[sign] = tile
        return result

    def pull(s, x, fixed, beyond, q):
        cx, cy, cz = LATTICE[q]
        at = x - cx + 1
        if fixed is not None and fixed - cx in (-1, nx):
            value = post[s, SLOT[q], at]
            if cz:
                value = pltpu.roll(value, cz % nz, 1)
            if cy:
                value = pltpu.roll(value, cy % ny, 0)
        elif cy or cz:
            value = mid[SLOT[q], at - 1]
        else:
            value = post[s, SLOT[q], at]
        if cy:
            j = MEMBERS[1, cy].index(q)
            edge = jnp.broadcast_to(ry[s, side(cy), j, at], (ny, nz))
            value = jnp.where(first_row if cy == 1 else last_row, edge, value)
        if cz:
            j = MEMBERS[2, cz].index(q)
            end = 0 if cz == 1 else nz - 1
            if fixed is not None and fixed - cx in (-1, nx):
                line = jnp.broadcast_to(rxz[s, side(cz), side(cx)], (ny, nz))
                outer = pltpu.roll(line, 0, 1, stride=1, stride_axis=0)
            else:
                outer = pltpu.roll(beyond[cz], lax.rem(end + nz - (x * FACE + j), nz), 1)
            value = jnp.where(first_lane if cz == 1 else last_lane, outer, value)
        return value

    def fresh(x, fixed):
        return collide([cur[q, x] for q in range(19)], [cur[q, x] for q in range(19, 26)], 1.0)

    advance(0, fresh, arrive, greet, 1.0 / KEEP_HEAT)

    def step(s, carry):
        scale, unit = carry
        receive(s)
        beyond = columns(s)

        def body(x, fixed):
            values = [pull(s, x, fixed, beyond, q) for q in range(26)]
            return collide(values[:19], values[19:], scale)

        unit = unit * (1.0 / KEEP_HEAT)
        advance(s + 1, body, lambda: None, lambda: None, unit)
        return scale * KEEP_HEAT, unit

    lax.fori_loop(0, STEPS - 1, step, (jnp.float32(KEEP_HEAT), jnp.float32(1.0 / KEEP_HEAT)))

    last = STEPS - 1
    receive(last)
    beyond = columns(last)

    def finish(x, fixed, flux):
        values = [pull(last, x, fixed, beyond, q) for q in range(26)]
        for q in range(26):
            result[q, x] = (KEEP_FLOW if q < 19 else KEEP_HEAT) ** STEPS * values[q]
        _, warmth, _, u = moments(values[:19], values[19:], KEEP_HEAT**STEPS)
        return flux + u[2] * warmth

    flux = jnp.zeros((ny, nz), jnp.float32)
    for x in (0, nx - 1):
        flux = finish(x, x, flux)
    flux = lax.fori_loop(1, nx - 1, lambda x, t: finish(x, None, t), flux, unroll=UNROLL)
    sums[me] = jnp.sum(flux, axis=0, keepdims=True)

    def send_sum(target):
        pltpu.make_async_remote_copy(
            src_ref=sums.at[me], dst_ref=sums.at[me],
            send_sem=sum_send, recv_sem=sum_recv, device_id=target,
        ).start()

    if joined:
        xs, ys = ([lax.rem(at + d, n) for d in range(n)] for at, n in zip((gx, gy), sizes))
        for k in range(count_z):
            z = jnp.where(2 * gz >= count_z, k, count_z - 1 - k)
            for dx in reversed(range(count_x)):
                for dy in reversed(range(count_y)):
                    there = {"gx": xs[dx], "gy": ys[dy], "gz": z}
                    if dx or dy:
                        send_sum(there)
                    else:
                        pl.when(z != gz)(functools.partial(send_sum, there))
    else:
        pl.loop(1, everyone)(lambda d: send_sum(ahead(d)))

    settle(send_sem.at[0], STEPS * rows(v for v in LINKS if v[2] == 0))
    for sign in SIDES:
        @pl.when(has[sign])
        def _():
            settle(send_sem.at[1 + side(sign)], STEPS * rows(v for v in LINKS if v[2] == sign))
    all_rows = pltpu.make_async_remote_copy(
        src_ref=sums.at[pl.ds(0, everyone - 1)], dst_ref=sums.at[pl.ds(0, everyone - 1)],
        send_sem=sum_send, recv_sem=sum_recv, device_id=ahead(1),
    )
    all_rows.wait_send()
    all_rows.wait_recv()
    result[26, 0, 0:1, :] = jnp.sum(sums[...], axis=0)


def write_out(scale, result, flow_out, heat_out, nusselt_out, small, sem):
    flow_cuts, heat_cuts = (0, 4, 8, 12, 16, 19), (0, 4, 7)
    for a, b in zip(flow_cuts, flow_cuts[1:]):
        pltpu.make_async_copy(result.at[a:b], flow_out.at[a:b], sem.at[0]).start()
    for a, b in zip(heat_cuts, heat_cuts[1:]):
        pltpu.make_async_copy(result.at[19 + a : 19 + b], heat_out.at[a:b], sem.at[0]).start()
    small[...] = 1.0 + scale * jnp.sum(result[26, 0, 0:1, :], axis=1, keepdims=True)
    number = pltpu.make_async_copy(small, nusselt_out, sem.at[1])
    number.start()
    pltpu.make_async_copy(result.at[0:26], result.at[0:26], sem.at[0]).wait()
    number.wait()


def per_device(sizes, flow_pops, heat_pops):
    nx, ny, nz = flow_pops.shape[1:]
    count_x, count_y, count_z = sizes
    f32 = jnp.float32
    dma = pltpu.SemaphoreType.DMA
    cells = nx * ny * nz * count_x * count_y * count_z
    scale = nz * count_z / (DIFFUSIVITY * (HOT_WALL - COLD_WALL)) / cells * KEEP_HEAT**STEPS
    hbm = pl.BlockSpec(memory_space=pltpu.HBM)
    vmem = pl.BlockSpec(memory_space=pltpu.VMEM)
    result = pl.pallas_call(
        functools.partial(kernel, sizes),
        out_shape=pltpu.VMEM((27, nx, ny, nz), f32),
        in_specs=[hbm, hbm],
        out_specs=vmem,
        scratch_shapes=[
            pltpu.VMEM((26, nx, ny, nz), f32),
            pltpu.VMEM((STEPS, 26, nx + 2, ny, nz), f32),
            pltpu.VMEM((26, nx, ny, nz), f32),
            pltpu.VMEM((STEPS, 2, FACE, nx + 2, 1, nz), f32),
            pltpu.VMEM((STEPS, 2, FACE, nx + 2, 1, nz), f32),
            pltpu.VMEM((STEPS, 2, ny, nz), f32),
            pltpu.VMEM((STEPS, 2, ny, nz), f32),
            pltpu.VMEM((STEPS, 2, 2, 1, nz), f32),
            pltpu.VMEM((STEPS, 2, 2, 1, nz), f32),
            pltpu.VMEM((STEPS, 2, 2, 1, nz), f32),
            pltpu.VMEM((STEPS, 2, 2, 1, nz), f32),
            pltpu.VMEM((count_x * count_y * count_z, 1, nz), f32),
            pltpu.VMEM((STEPS * 2 * (FACE * (nx + ny) + 2), 1, nz), f32),
            dma((3,)),
            dma((3,)),
            dma((STEPS, 3)),
            dma,
            dma,
        ],
        compiler_params=pltpu.CompilerParams(
            collective_id=0, has_side_effects=True, vmem_limit_bytes=55000000
        ),
    )(pltpu.with_memory_space_constraint(flow_pops, pltpu.HBM), pltpu.with_memory_space_constraint(heat_pops, pltpu.HBM))
    flow, heat, nusselt = pl.pallas_call(
        functools.partial(write_out, scale),
        out_shape=(
            jax.ShapeDtypeStruct(flow_pops.shape, f32),
            jax.ShapeDtypeStruct(heat_pops.shape, f32),
            jax.ShapeDtypeStruct((1, 1), f32),
        ),
        in_specs=[vmem],
        out_specs=(hbm, hbm, hbm),
        scratch_shapes=[pltpu.VMEM((1, 1), f32), dma((2,))],
        compiler_params=pltpu.CompilerParams(vmem_limit_bytes=1024 * 1024),
    )(result)
    return flow, heat, nusselt.reshape(())


def solution(mesh):
    placed = P(None, "gx", "gy", "gz")
    sizes = tuple(mesh.shape[a] for a in ("gx", "gy", "gz"))
    return jax.shard_map(
        functools.partial(per_device, sizes),
        mesh=mesh,
        in_specs=(placed, placed),
        out_specs=(placed, placed, P()),
        check_vma=False,
    )
```

```python
import functools

import jax
import jax.numpy as jnp
import numpy as np
from jax import lax
from jax.experimental import pallas as pl
from jax.experimental.pallas import tpu as pltpu
from jax.sharding import PartitionSpec as P

STEPS = 3

FLOW_SET = np.array(
    [
        [0, 0, 0],
        [1, 0, 0],
        [-1, 0, 0],
        [0, 1, 0],
        [0, -1, 0],
        [0, 0, 1],
        [0, 0, -1],
        [1, 1, 0],
        [-1, -1, 0],
        [1, -1, 0],
        [-1, 1, 0],
        [1, 0, 1],
        [-1, 0, -1],
        [1, 0, -1],
        [-1, 0, 1],
        [0, 1, 1],
        [0, -1, -1],
        [0, 1, -1],
        [0, -1, 1],
    ]
)
FLOW_WEIGHT = np.array([1.0 / 3.0] + [1.0 / 18.0] * 6 + [1.0 / 36.0] * 12)
HEAT_WEIGHT = np.array([0.25] + [0.125] * 6)
LATTICE = [tuple(int(c) for c in v) for v in np.concatenate([FLOW_SET, FLOW_SET[:7]], axis=0)]
WEIGHTS = [float(w) for w in np.concatenate([FLOW_WEIGHT, HEAT_WEIGHT])]
OPPOSITE = (
    [0]
    + [q + 1 if q % 2 else q - 1 for q in range(1, 19)]
    + [19]
    + [q - 1 if q % 2 else q + 1 for q in range(20, 26)]
)
TAU_FLOW = 0.6
TAU_HEAT = 0.7
GRAVITY_LIFT = 0.01
HOT_WALL = 0.5
COLD_WALL = -0.5
DIFFUSIVITY = (TAU_HEAT - 0.5) / 4.0
KEEP_FLOW = 1.0 - 1.0 / TAU_FLOW
KEEP_HEAT = 1.0 - 1.0 / TAU_HEAT

MEMBERS = {
    (axis, sign): [q for q in range(26) if LATTICE[q][axis] == sign]
    for axis in range(3)
    for sign in (1, -1)
}
FACE = len(MEMBERS[0, 1])
STORED = (
    MEMBERS[0, 1] + MEMBERS[0, -1] + [q for q in range(26) if LATTICE[q][0] == 0]
)
SLOT = [STORED.index(q) for q in range(26)]
SIDES = (1, -1)
UNROLL = True
LINKS = sorted({v for v in LATTICE if v != (0, 0, 0)})


EARLY = sorted([v for v in LINKS if v[0]], key=lambda v: sum(abs(c) for c in v))
LATE = sorted([v for v in LINKS if not v[0]], key=lambda v: -sum(abs(c) for c in v))


def group(v):
    return 0 if v[2] == 0 else 1 + side(v[2])


def side(sign):
    return 0 if sign == 1 else 1


def total(terms):
    terms = list(terms)
    while len(terms) > 1:
        terms = [a + b for a, b in zip(terms[::2], terms[1::2])] + terms[len(terms) & ~1 :]
    return terms[0]


def gather(values, span):
    flat = [values[q - span[0]] for q in span if LATTICE[q][2] == 0]
    tilted = [values[q - span[0]] for q in span if LATTICE[q][2]]
    return total(flat) + total(tilted)


def moments(f, g, scale):
    rho, warmth = gather(f, range(19)), gather(g, range(19, 26))
    flow = []
    for axis in range(3):
        result = None
        for q in sorted(range(1, 19, 2), key=lambda q: abs(LATTICE[q][2])):
            if LATTICE[q][axis]:
                odd = f[q] - f[q + 1]
                if result is None:
                    result = odd
                else:
                    result = result + odd if LATTICE[q][axis] == 1 else result - odd
        flow.append(result)
    half = (0.5 * GRAVITY_LIFT * scale) * warmth
    inv = 1.0 / rho
    return rho, warmth, half, (flow[0] * inv, flow[1] * inv, flow[2] * inv + half)


def collide(f, g, scale):
    rho, warmth, half, u = moments(f, g, scale)
    push = rho * half
    rate = 1.0 / TAU_FLOW
    lift = 2.0 * (1.0 - 0.5 / TAU_FLOW)
    weight = WEIGHTS[7] / KEEP_FLOW
    square = u[0] * u[0] + u[1] * u[1] + u[2] * u[2]
    base = (weight * rate * rho) * (1.0 - 1.5 * square) - (3.0 * lift * weight) * (u[2] * push)
    quad = (4.5 * rate * weight) * rho
    line = (3.0 * rate * weight) * rho
    push3 = (3.0 * lift * weight) * push
    push9 = (9.0 * lift * weight) * push
    small = (base, quad, line, push3, push9)
    large = tuple((WEIGHTS[1] / WEIGHTS[7]) * part for part in small)
    post = [None] * 26
    post[0] = f[0] + (WEIGHTS[0] / WEIGHTS[7]) * base
    for q in range(1, 19, 2):
        c = LATTICE[q]
        along = None
        for axis in range(3):
            if c[axis]:
                if along is None:
                    along = u[axis]
                else:
                    along = along + u[axis] if c[axis] == 1 else along - u[axis]
        base, quad, line, push3, push9 = large if q < 7 else small
        inner = quad * along
        odd = line * along
        if c[2] == 1:
            inner, odd = inner + push9, odd + push3
        elif c[2] == -1:
            inner, odd = inner - push9, odd - push3
        even = base + along * inner
        post[q] = f[q] + (even + odd)
        post[q + 1] = f[q + 1] + (even - odd)
    share = 1.0 / (TAU_HEAT * KEEP_HEAT)
    post[19] = g[0] + (WEIGHTS[19] * share) * warmth
    still = (WEIGHTS[20] * share) * warmth
    slope = (4.0 * WEIGHTS[20] * share) * warmth
    for axis in range(3):
        drift = slope * u[axis]
        q = 20 + 2 * axis
        post[q] = g[q - 19] + (still + drift)
        post[q + 1] = g[q - 18] + (still - drift)
    return post


def kernel(
    sizes, flow_in, heat_in, result,
    cur, post, mid, sx, rx, sy, ry, sz, rz, sxz, rxz, syz, ryz, sums, ledger,
    in_sem, send_sem, recv_sem, sum_send, sum_recv,
):
    count_x, count_y, count_z = sizes
    nx, ny, nz = cur.shape[1:]
    gx, gy, gz = (lax.axis_index(a) for a in ("gx", "gy", "gz"))
    has = {1: gz < count_z - 1, -1: gz > 0}
    everyone = count_x * count_y * count_z
    me = (gx * count_y + gy) * count_z + gz

    def device(v):
        return {
            "gx": lax.rem(gx + v[0] + count_x, count_x),
            "gy": lax.rem(gy + v[1] + count_y, count_y),
            "gz": gz + v[2],
        }

    def ahead(distance):
        other = lax.rem(me + distance, everyone)
        row = other // count_z
        return {"gx": row // count_y, "gy": lax.rem(row, count_y), "gz": lax.rem(other, count_z)}

    def load(part, x):
        return (
            pltpu.make_async_copy(flow_in.at[:, x], cur.at[0:19, x], in_sem.at[part]),
            pltpu.make_async_copy(heat_in.at[:, x], cur.at[19:26, x], in_sem.at[part]),
        )

    def pieces(part, x):
        cuts = (0, 7, 13, 19)
        return [
            pltpu.make_async_copy(flow_in.at[a:b, x], cur.at[a:b, x], in_sem.at[part])
            for a, b in zip(cuts, cuts[1:])
        ] + [pltpu.make_async_copy(heat_in.at[:, x], cur.at[19:26, x], in_sem.at[part])]

    loads = [pieces(0, 0), pieces(1, nx - 1), [c for x in range(1, nx - 1) for c in load(2, x)]]
    def fetch(parts):
        for copies in parts:
            for copy in copies:
                copy.start()

    fetch(loads[:2])
    barrier = pltpu.get_barrier_semaphore()
    near = sorted(
        {(v[0] % count_x, v[1] % count_y, v[2]) for v in LINKS}, key=lambda v: -sum(c != 0 for c in v)
    )
    reach = (count_x // 2, count_y // 2, count_z - 1)
    joined = max(reach) <= STEPS and sum(reach) <= 2 * STEPS
    if joined:
        for sign in SIDES:
            @pl.when(has[sign])
            def _():
                for v in near:
                    if v[2] == sign:
                        pl.semaphore_signal(barrier, inc=1, device_id=device(v))
        for v in near:
            if v[2] == 0:
                pl.semaphore_signal(barrier, inc=1, device_id=device(v))
    else:
        @pl.loop(1, everyone)
        def _(d):
            pl.semaphore_signal(barrier, inc=1, device_id=ahead(d))
    fetch(loads[2:])

    def greet():
        if joined:
            count = len([v for v in near if v[2] == 0])
            for sign in SIDES:
                count += jnp.where(has[sign], len([v for v in near if v[2] == sign]), 0)
        else:
            count = everyone - 1
        pl.semaphore_wait(barrier, count)

    lane = lax.broadcasted_iota(jnp.int32, (ny, nz), 1)
    row = lax.broadcasted_iota(jnp.int32, (ny, nz), 0)
    first_row, last_row = row == 0, row == ny - 1
    first_lane, last_lane = lane == 0, lane == nz - 1
    place = lax.rem(lane, FACE)
    slant = {1: lane == lax.rem(nz - row, nz), -1: lane == nz - 1 - row}

    def lanes_of(sign, pick):
        mask = None
        for j, q in enumerate(MEMBERS[2, sign]):
            if pick(q):
                mask = place == j if mask is None else mask | (place == j)
        return mask

    paired = count_x == 2

    def message(s, v):
        x, y, z = v
        if z == 0:
            start = 0 if x == 1 else FACE
            edge, halo = (nx, 0) if x == 1 else (1, nx + 1)
            if y == 0:
                src, dst = (sx.at[s], rx.at[s]) if paired else (sx.at[s, side(x)], rx.at[s, side(x)])
            elif x == 0:
                src = sy.at[s, side(y), :, 1 : nx + 1]
                dst = ry.at[s, side(y), :, 1 : nx + 1]
            else:
                j = MEMBERS[1, y].index(LATTICE.index(v))
                src = sy.at[s, side(y), j, edge]
                dst = ry.at[s, side(y), j, halo]
        elif y == 0:
            if x == 0:
                src, dst = sz.at[s, side(z)], rz.at[s, side(z)]
            elif paired:
                src, dst = sxz.at[s, side(z)], rxz.at[s, side(z)]
            else:
                src, dst = sxz.at[s, side(z), side(x)], rxz.at[s, side(z), side(x)]
        else:
            src = syz.at[s, side(z), side(y)]
            dst = ryz.at[s, side(z), side(y)]
        return pltpu.make_async_remote_copy(
            src_ref=src, dst_ref=dst, send_sem=send_sem.at[group(v)], recv_sem=recv_sem.at[s, group(v)],
            device_id=device(v),
        )

    def send(s, links):
        links = [v for v in links if not (paired and v[0] == -1 and v[1] == 0)]
        for v in links:
            if v[2] == 0:
                message(s, v).start()
        for sign in SIDES:
            if any(v[2] == sign for v in links):
                @pl.when(has[sign])
                def _():
                    for v in links:
                        if v[2] == sign:
                            message(s, v).start()

    def rows(links):
        count = 0
        for x, y, z in links:
            if y == 0:
                count += FACE * ny if z == 0 else ny if x == 0 else 1
            else:
                count += FACE * nx if x == 0 and z == 0 else 1
        return count

    def settle(sem, count):
        pltpu.make_async_copy(ledger.at[0:count], ledger.at[0:count], sem).wait()

    def receive(s):
        settle(recv_sem.at[s, 0], rows(v for v in LINKS if v[2] == 0))
        for sign in SIDES:
            @pl.when(has[-sign])
            def _():
                settle(recv_sem.at[s, 1 + side(sign)], rows(v for v in LINKS if v[2] == sign))

    def flatten(sign, tile, at):
        column = jnp.broadcast_to(tile[:, at : at + 1], (ny, nz))
        return jnp.sum(jnp.where(slant[sign], column, 0.0), axis=0, keepdims=True)

    def target(x, q):
        return lax.rem(x + (LATTICE[q][0] + nx), nx) * FACE

    def keep_urgent(s, x, way, values):
        for j, q in enumerate(MEMBERS[0, way]):
            sx[s, side(way), j] = values[q]
        for y in SIDES:
            q = LATTICE.index((way, y, 0))
            r = ny - 1 if y == 1 else 0
            sy[s, side(y), MEMBERS[1, y].index(q), x + 1] = values[q][r : r + 1, :]

    def keep_plane(s, x, way, values, packs):
        for q in range(26):
            if LATTICE[q][0] != way:
                post[s, SLOT[q], x + 1] = values[q]
        for sign in SIDES:
            r = ny - 1 if sign == 1 else 0
            for j, q in enumerate(MEMBERS[1, sign]):
                if LATTICE[q][0] == way:
                    continue
                value = values[q]
                if LATTICE[q][2]:
                    value = pltpu.roll(value, LATTICE[q][2] % nz, 1)
                sy[s, side(sign), j, x + 1] = value[r : r + 1, :]
        new = []
        for sign, pack in zip(SIDES, packs):
            source = nz - 1 if sign == 1 else 0
            for j, q in enumerate(MEMBERS[2, sign]):
                k = target(x, q) + j
                turned = pltpu.roll(values[q], lax.rem(k + (nz - source), nz), 1)
                pack = jnp.where(lane == k, turned, pack)
            new.append(pack)
        return tuple(new)

    def stream(s, x):
        for q in range(26):
            cx, cy, cz = LATTICE[q]
            if cy or cz:
                value = post[s, SLOT[q], x + 1]
                if cz:
                    value = pltpu.roll(value, cz % nz, 1)
                if cy:
                    value = pltpu.roll(value, cy % ny, 0)
                mid[SLOT[q], x] = value

    def bounce(s, sign, pack, unit):
        own = MEMBERS[2, sign]
        edge = (nx - 1) * FACE
        wall = pack
        for x in SIDES:
            near_part = pltpu.roll(pack, (-x * FACE) % nz, 1)
            far_part = pltpu.roll(pack, (x * edge) % nz, 1)
            far = lane >= edge if x == 1 else lane < FACE
            wall = jnp.where(
                lanes_of(sign, lambda q: LATTICE[q][0] == x), jnp.where(far, far_part, near_part), wall
            )
        for y in SIDES:
            wall = jnp.where(
                lanes_of(sign, lambda q: LATTICE[q][1] == y), pltpu.roll(pack, -y % ny, 0), wall
            )
        weight = WEIGHTS[own[-1]]
        warm = (2.0 * weight * (COLD_WALL if sign == 1 else HOT_WALL)) * unit
        wall = jnp.where(lanes_of(sign, lambda q: q >= 19), warm - wall, wall)
        rz[s, side(-sign)] = wall
        for x in SIDES:
            q = LATTICE.index((x, 0, -sign))
            at = (0 if x == 1 else nx - 1) * FACE + MEMBERS[2, -sign].index(q)
            rxz[s, side(-sign), side(x)] = flatten(-sign, wall, at)

    def arrive():
        planes = ((0, cur.at[:, 0]), (1, cur.at[:, nx - 1]), (2, cur.at[:, 1 : nx - 1]))
        for part, planes_of in planes:
            pltpu.make_async_copy(planes_of, planes_of, in_sem.at[part]).wait()
            if part:
                yield

    def advance(s, body, arrive, before_send, unit):
        zero = jnp.zeros((ny, nz), jnp.float32)
        packs = (zero, zero)
        stages = iter(arrive() or ())
        next(stages, None)
        first = []
        for x, way in ((0, -1), (nx - 1, 1)):
            values = body(x, x)
            first.append((x, way, values))
            keep_urgent(s, x, way, values)
        before_send()
        send(s, [v for v in EARLY if v[1]])
        send(s, [v for v in EARLY if not v[1] and not v[2]])
        for x, way, values in first:
            for sign in SIDES:
                value = values[LATTICE.index((way, 0, sign))]
                sxz[s, side(sign), side(way)] = flatten(sign, value, nz - 1 if sign == 1 else 0)
        send(s, [v for v in EARLY if v[2]])
        for x, way, values in first:
            packs = keep_plane(s, x, way, values, packs)
        next(stages, None)
        packs = lax.fori_loop(
            1, nx - 1, lambda x, p: keep_plane(s, x, None, body(x, None), p), packs, unroll=UNROLL
        )
        send(s, [v for v in LATE if v[2] == 0])
        for sign, pack in zip(SIDES, packs):
            whole = pack
            for y in SIDES:
                whole = jnp.where(
                    lanes_of(sign, lambda q: LATTICE[q][1] == y), pltpu.roll(pack, y % ny, 0), whole
                )
            sz[s, side(sign)] = whole
            for y in SIDES:
                r = 0 if y == 1 else ny - 1
                syz[s, side(sign), side(y)] = whole[r : r + 1, :]
        send(s, [v for v in LATE if v[2]])
        for sign in SIDES:
            @pl.when(jnp.logical_not(has[sign]))
            def _():
                bounce(s, sign, sz[s, side(sign)], unit)
        lax.fori_loop(0, nx, lambda x, c: (stream(s, x), c)[1], 0, unroll=2)

    def columns(s):
        result = {}
        for sign in SIDES:
            tile = rz[s, side(sign)]
            for y in SIDES:
                mask = lanes_of(sign, lambda q: LATTICE[q][1] == y) & (first_row if y == 1 else last_row)
                edge = jnp.broadcast_to(ryz[s, side(sign), side(y)], (ny, nz))
                tile = jnp.where(mask & has[-sign], edge, tile)
            result[sign] = tile
        return result

    def pull(s, x, fixed, beyond, q):
        cx, cy, cz = LATTICE[q]
        at = x - cx + 1
        if fixed is not None and fixed - cx in (-1, nx):
            value = rx[s, side(cx), MEMBERS[0, cx].index(q)]
            if cz:
                value = pltpu.roll(value, cz % nz, 1)
            if cy:
                value = pltpu.roll(value, cy % ny, 0)
        elif cy or cz:
            value = mid[SLOT[q], at - 1]
        else:
            value = post[s, SLOT[q], at]
        if cy:
            j = MEMBERS[1, cy].index(q)
            edge = jnp.broadcast_to(ry[s, side(cy), j, at], (ny, nz))
            value = jnp.where(first_row if cy == 1 else last_row, edge, value)
        if cz:
            j = MEMBERS[2, cz].index(q)
            end = 0 if cz == 1 else nz - 1
            if fixed is not None and fixed - cx in (-1, nx):
                line = jnp.broadcast_to(rxz[s, side(cz), side(cx)], (ny, nz))
                outer = pltpu.roll(line, 0, 1, stride=1, stride_axis=0)
            else:
                outer = pltpu.roll(beyond[cz], lax.rem(end + nz - (x * FACE + j), nz), 1)
            value = jnp.where(first_lane if cz == 1 else last_lane, outer, value)
        return value

    def fresh(x, fixed):
        return collide([cur[q, x] for q in range(19)], [cur[q, x] for q in range(19, 26)], 1.0)

    advance(0, fresh, arrive, greet, 1.0 / KEEP_HEAT)

    def step(s, carry):
        scale, unit = carry
        receive(s)
        beyond = columns(s)

        def body(x, fixed):
            values = [pull(s, x, fixed, beyond, q) for q in range(26)]
            return collide(values[:19], values[19:], scale)

        unit = unit * (1.0 / KEEP_HEAT)
        advance(s + 1, body, lambda: None, lambda: None, unit)
        return scale * KEEP_HEAT, unit

    lax.fori_loop(0, STEPS - 1, step, (jnp.float32(KEEP_HEAT), jnp.float32(1.0 / KEEP_HEAT)))

    last = STEPS - 1
    receive(last)
    beyond = columns(last)

    def finish(x, fixed, flux):
        values = [pull(last, x, fixed, beyond, q) for q in range(26)]
        for q in range(26):
            result[q, x] = (KEEP_FLOW if q < 19 else KEEP_HEAT) ** STEPS * values[q]
        _, warmth, _, u = moments(values[:19], values[19:], KEEP_HEAT**STEPS)
        return flux + u[2] * warmth

    flux = jnp.zeros((ny, nz), jnp.float32)
    for x in (0, nx - 1):
        flux = finish(x, x, flux)
    flux = lax.fori_loop(1, nx - 1, lambda x, t: finish(x, None, t), flux, unroll=UNROLL)
    sums[me] = jnp.sum(flux, axis=0, keepdims=True)

    def send_sum(target):
        pltpu.make_async_remote_copy(
            src_ref=sums.at[me], dst_ref=sums.at[me],
            send_sem=sum_send, recv_sem=sum_recv, device_id=target,
        ).start()

    if joined:
        xs, ys = ([lax.rem(at + d, n) for d in range(n)] for at, n in zip((gx, gy), sizes))
        for k in range(count_z):
            z = jnp.where(2 * gz >= count_z, k, count_z - 1 - k)
            for dx in reversed(range(count_x)):
                for dy in reversed(range(count_y)):
                    there = {"gx": xs[dx], "gy": ys[dy], "gz": z}
                    if dx or dy:
                        send_sum(there)
                    else:
                        pl.when(z != gz)(functools.partial(send_sum, there))
    else:
        pl.loop(1, everyone)(lambda d: send_sum(ahead(d)))

    settle(send_sem.at[0], STEPS * rows(v for v in LINKS if v[2] == 0))
    for sign in SIDES:
        @pl.when(has[sign])
        def _():
            settle(send_sem.at[1 + side(sign)], STEPS * rows(v for v in LINKS if v[2] == sign))
    all_rows = pltpu.make_async_remote_copy(
        src_ref=sums.at[pl.ds(0, everyone - 1)], dst_ref=sums.at[pl.ds(0, everyone - 1)],
        send_sem=sum_send, recv_sem=sum_recv, device_id=ahead(1),
    )
    all_rows.wait_send()
    all_rows.wait_recv()
    result[26, 0, 0:1, :] = jnp.sum(sums[...], axis=0)


def write_out(scale, result, flow_out, heat_out, nusselt_out, small, sem):
    flow_cuts, heat_cuts = (0, 4, 8, 12, 16, 19), (0, 4, 7)
    for a, b in zip(flow_cuts, flow_cuts[1:]):
        pltpu.make_async_copy(result.at[a:b], flow_out.at[a:b], sem.at[0]).start()
    for a, b in zip(heat_cuts, heat_cuts[1:]):
        pltpu.make_async_copy(result.at[19 + a : 19 + b], heat_out.at[a:b], sem.at[0]).start()
    small[...] = 1.0 + scale * jnp.sum(result[26, 0, 0:1, :], axis=1, keepdims=True)
    number = pltpu.make_async_copy(small, nusselt_out, sem.at[1])
    number.start()
    pltpu.make_async_copy(result.at[0:26], result.at[0:26], sem.at[0]).wait()
    number.wait()


def per_device(sizes, flow_pops, heat_pops):
    nx, ny, nz = flow_pops.shape[1:]
    count_x, count_y, count_z = sizes
    f32 = jnp.float32
    dma = pltpu.SemaphoreType.DMA
    cells = nx * ny * nz * count_x * count_y * count_z
    scale = nz * count_z / (DIFFUSIVITY * (HOT_WALL - COLD_WALL)) / cells * KEEP_HEAT**STEPS
    hbm = pl.BlockSpec(memory_space=pltpu.HBM)
    vmem = pl.BlockSpec(memory_space=pltpu.VMEM)
    result = pl.pallas_call(
        functools.partial(kernel, sizes),
        out_shape=pltpu.VMEM((27, nx, ny, nz), f32),
        in_specs=[hbm, hbm],
        out_specs=vmem,
        scratch_shapes=[
            pltpu.VMEM((26, nx, ny, nz), f32),
            pltpu.VMEM((STEPS, 26, nx + 2, ny, nz), f32),
            pltpu.VMEM((26, nx, ny, nz), f32),
            pltpu.VMEM((STEPS, 2, FACE, ny, nz), f32),
            pltpu.VMEM((STEPS, 2, FACE, ny, nz), f32),
            pltpu.VMEM((STEPS, 2, FACE, nx + 2, 1, nz), f32),
            pltpu.VMEM((STEPS, 2, FACE, nx + 2, 1, nz), f32),
            pltpu.VMEM((STEPS, 2, ny, nz), f32),
            pltpu.VMEM((STEPS, 2, ny, nz), f32),
            pltpu.VMEM((STEPS, 2, 2, 1, nz), f32),
            pltpu.VMEM((STEPS, 2, 2, 1, nz), f32),
            pltpu.VMEM((STEPS, 2, 2, 1, nz), f32),
            pltpu.VMEM((STEPS, 2, 2, 1, nz), f32),
            pltpu.VMEM((count_x * count_y * count_z, 1, nz), f32),
            pltpu.VMEM((STEPS * 2 * (FACE * (nx + ny) + 2), 1, nz), f32),
            dma((3,)),
            dma((3,)),
            dma((STEPS, 3)),
            dma,
            dma,
        ],
        compiler_params=pltpu.CompilerParams(
            collective_id=0, has_side_effects=True, vmem_limit_bytes=55000000
        ),
    )(pltpu.with_memory_space_constraint(flow_pops, pltpu.HBM), pltpu.with_memory_space_constraint(heat_pops, pltpu.HBM))
    flow, heat, nusselt = pl.pallas_call(
        functools.partial(write_out, scale),
        out_shape=(
            jax.ShapeDtypeStruct(flow_pops.shape, f32),
            jax.ShapeDtypeStruct(heat_pops.shape, f32),
            jax.ShapeDtypeStruct((1, 1), f32),
        ),
        in_specs=[vmem],
        out_specs=(hbm, hbm, hbm),
        scratch_shapes=[pltpu.VMEM((1, 1), f32), dma((2,))],
        compiler_params=pltpu.CompilerParams(vmem_limit_bytes=1024 * 1024),
    )(result)
    return flow, heat, nusselt.reshape(())


def solution(mesh):
    placed = P(None, "gx", "gy", "gz")
    sizes = tuple(mesh.shape[a] for a in ("gx", "gy", "gz"))
    return jax.shard_map(
        functools.partial(per_device, sizes),
        mesh=mesh,
        in_specs=(placed, placed),
        out_specs=(placed, placed, P()),
        check_vma=False,
    )
```

```python
import functools

import jax
import jax.numpy as jnp
import numpy as np
from jax import lax
from jax.experimental import pallas as pl
from jax.experimental.pallas import tpu as pltpu
from jax.sharding import PartitionSpec as P

STEPS = 3

FLOW_SET = np.array(
    [
        [0, 0, 0],
        [1, 0, 0],
        [-1, 0, 0],
        [0, 1, 0],
        [0, -1, 0],
        [0, 0, 1],
        [0, 0, -1],
        [1, 1, 0],
        [-1, -1, 0],
        [1, -1, 0],
        [-1, 1, 0],
        [1, 0, 1],
        [-1, 0, -1],
        [1, 0, -1],
        [-1, 0, 1],
        [0, 1, 1],
        [0, -1, -1],
        [0, 1, -1],
        [0, -1, 1],
    ]
)
FLOW_WEIGHT = np.array([1.0 / 3.0] + [1.0 / 18.0] * 6 + [1.0 / 36.0] * 12)
HEAT_WEIGHT = np.array([0.25] + [0.125] * 6)
LATTICE = [tuple(int(c) for c in v) for v in np.concatenate([FLOW_SET, FLOW_SET[:7]], axis=0)]
WEIGHTS = [float(w) for w in np.concatenate([FLOW_WEIGHT, HEAT_WEIGHT])]
OPPOSITE = (
    [0]
    + [q + 1 if q % 2 else q - 1 for q in range(1, 19)]
    + [19]
    + [q - 1 if q % 2 else q + 1 for q in range(20, 26)]
)
TAU_FLOW = 0.6
TAU_HEAT = 0.7
GRAVITY_LIFT = 0.01
HOT_WALL = 0.5
COLD_WALL = -0.5
DIFFUSIVITY = (TAU_HEAT - 0.5) / 4.0
KEEP_FLOW = 1.0 - 1.0 / TAU_FLOW
KEEP_HEAT = 1.0 - 1.0 / TAU_HEAT

MEMBERS = {
    (axis, sign): [q for q in range(26) if LATTICE[q][axis] == sign]
    for axis in range(3)
    for sign in (1, -1)
}
FACE = len(MEMBERS[0, 1])
STORED = (
    MEMBERS[0, 1] + MEMBERS[0, -1] + [q for q in range(26) if LATTICE[q][0] == 0]
)
SLOT = [STORED.index(q) for q in range(26)]
SIDES = (1, -1)
UNROLL = True
LINKS = sorted({v for v in LATTICE if v != (0, 0, 0)})


EARLY = sorted([v for v in LINKS if v[0]], key=lambda v: sum(abs(c) for c in v))
LATE = sorted([v for v in LINKS if not v[0]], key=lambda v: -sum(abs(c) for c in v))


def group(v):
    return 0 if v[2] == 0 else 1 + side(v[2])


def side(sign):
    return 0 if sign == 1 else 1


def total(terms):
    terms = list(terms)
    while len(terms) > 1:
        terms = [a + b for a, b in zip(terms[::2], terms[1::2])] + terms[len(terms) & ~1 :]
    return terms[0]


def gather(values, span):
    flat = [values[q - span[0]] for q in span if LATTICE[q][2] == 0]
    tilted = [values[q - span[0]] for q in span if LATTICE[q][2]]
    return total(flat) + total(tilted)


def moments(f, g, scale):
    rho, warmth = gather(f, range(19)), gather(g, range(19, 26))
    flow = []
    for axis in range(3):
        result = None
        for q in sorted(range(1, 19, 2), key=lambda q: abs(LATTICE[q][2])):
            if LATTICE[q][axis]:
                odd = f[q] - f[q + 1]
                if result is None:
                    result = odd
                else:
                    result = result + odd if LATTICE[q][axis] == 1 else result - odd
        flow.append(result)
    half = (0.5 * GRAVITY_LIFT * scale) * warmth
    inv = 1.0 / rho
    return rho, warmth, half, (flow[0] * inv, flow[1] * inv, flow[2] * inv + half)


def collide(f, g, scale):
    rho, warmth, half, u = moments(f, g, scale)
    push = rho * half
    rate = 1.0 / TAU_FLOW
    lift = 2.0 * (1.0 - 0.5 / TAU_FLOW)
    weight = WEIGHTS[7] / KEEP_FLOW
    square = u[0] * u[0] + u[1] * u[1] + u[2] * u[2]
    base = (weight * rate * rho) * (1.0 - 1.5 * square) - (3.0 * lift * weight) * (u[2] * push)
    quad = (4.5 * rate * weight) * rho
    line = (3.0 * rate * weight) * rho
    push3 = (3.0 * lift * weight) * push
    push9 = (9.0 * lift * weight) * push
    small = (base, quad, line, push3, push9)
    large = tuple((WEIGHTS[1] / WEIGHTS[7]) * part for part in small)
    post = [None] * 26
    post[0] = f[0] + (WEIGHTS[0] / WEIGHTS[7]) * base
    for q in range(1, 19, 2):
        c = LATTICE[q]
        along = None
        for axis in range(3):
            if c[axis]:
                if along is None:
                    along = u[axis]
                else:
                    along = along + u[axis] if c[axis] == 1 else along - u[axis]
        base, quad, line, push3, push9 = large if q < 7 else small
        inner = quad * along
        odd = line * along
        if c[2] == 1:
            inner, odd = inner + push9, odd + push3
        elif c[2] == -1:
            inner, odd = inner - push9, odd - push3
        even = base + along * inner
        post[q] = f[q] + (even + odd)
        post[q + 1] = f[q + 1] + (even - odd)
    share = 1.0 / (TAU_HEAT * KEEP_HEAT)
    post[19] = g[0] + (WEIGHTS[19] * share) * warmth
    still = (WEIGHTS[20] * share) * warmth
    slope = (4.0 * WEIGHTS[20] * share) * warmth
    for axis in range(3):
        drift = slope * u[axis]
        q = 20 + 2 * axis
        post[q] = g[q - 19] + (still + drift)
        post[q + 1] = g[q - 18] + (still - drift)
    return post


def kernel(
    sizes, flow_in, heat_in, result,
    cur, post, mid, sx, rx, sy, ry, sz, rz, sxy, rxy, sxz, rxz, syz, ryz, sums, ledger,
    in_sem, send_sem, recv_sem, sum_send, sum_recv,
):
    count_x, count_y, count_z = sizes
    nx, ny, nz = cur.shape[1:]
    gx, gy, gz = (lax.axis_index(a) for a in ("gx", "gy", "gz"))
    has = {1: gz < count_z - 1, -1: gz > 0}
    everyone = count_x * count_y * count_z
    me = (gx * count_y + gy) * count_z + gz

    def device(v):
        return {
            "gx": lax.rem(gx + v[0] + count_x, count_x),
            "gy": lax.rem(gy + v[1] + count_y, count_y),
            "gz": gz + v[2],
        }

    def ahead(distance):
        other = lax.rem(me + distance, everyone)
        row = other // count_z
        return {"gx": row // count_y, "gy": lax.rem(row, count_y), "gz": lax.rem(other, count_z)}

    def load(part, x):
        return (
            pltpu.make_async_copy(flow_in.at[:, x], cur.at[0:19, x], in_sem.at[part]),
            pltpu.make_async_copy(heat_in.at[:, x], cur.at[19:26, x], in_sem.at[part]),
        )

    def pieces(part, x):
        cuts = (0, 7, 13, 19)
        return [
            pltpu.make_async_copy(flow_in.at[a:b, x], cur.at[a:b, x], in_sem.at[part])
            for a, b in zip(cuts, cuts[1:])
        ] + [pltpu.make_async_copy(heat_in.at[:, x], cur.at[19:26, x], in_sem.at[part])]

    loads = [pieces(0, 0), pieces(1, nx - 1), [c for x in range(1, nx - 1) for c in load(2, x)]]
    def fetch(parts):
        for copies in parts:
            for copy in copies:
                copy.start()

    fetch(loads[:2])
    barrier = pltpu.get_barrier_semaphore()
    near = sorted(
        {(v[0] % count_x, v[1] % count_y, v[2]) for v in LINKS}, key=lambda v: -sum(c != 0 for c in v)
    )
    reach = (count_x // 2, count_y // 2, count_z - 1)
    joined = max(reach) <= STEPS and sum(reach) <= 2 * STEPS
    if joined:
        for sign in SIDES:
            @pl.when(has[sign])
            def _():
                for v in near:
                    if v[2] == sign:
                        pl.semaphore_signal(barrier, inc=1, device_id=device(v))
        for v in near:
            if v[2] == 0:
                pl.semaphore_signal(barrier, inc=1, device_id=device(v))
    else:
        @pl.loop(1, everyone)
        def _(d):
            pl.semaphore_signal(barrier, inc=1, device_id=ahead(d))
    fetch(loads[2:])

    def greet():
        if joined:
            count = len([v for v in near if v[2] == 0])
            for sign in SIDES:
                count += jnp.where(has[sign], len([v for v in near if v[2] == sign]), 0)
        else:
            count = everyone - 1
        pl.semaphore_wait(barrier, count)

    lane = lax.broadcasted_iota(jnp.int32, (ny, nz), 1)
    row = lax.broadcasted_iota(jnp.int32, (ny, nz), 0)
    first_row, last_row = row == 0, row == ny - 1
    first_lane, last_lane = lane == 0, lane == nz - 1
    place = lax.rem(lane, FACE)
    slant = {1: lane == lax.rem(nz - row, nz), -1: lane == nz - 1 - row}

    def lanes_of(sign, pick):
        mask = None
        for j, q in enumerate(MEMBERS[2, sign]):
            if pick(q):
                mask = place == j if mask is None else mask | (place == j)
        return mask

    paired = count_x == 2

    def message(s, v):
        x, y, z = v
        if z == 0:
            if y == 0:
                src, dst = (sx.at[s], rx.at[s]) if paired else (sx.at[s, side(x)], rx.at[s, side(x)])
            elif x == 0:
                src = sy.at[s, side(y), :, 1 : nx + 1]
                dst = ry.at[s, side(y), :, 1 : nx + 1]
            else:
                src, dst = sxy.at[s, side(y)], rxy.at[s, side(y)]
                if not paired:
                    src, dst = src.at[side(x)], dst.at[side(x)]
        elif y == 0:
            if x == 0:
                src, dst = sz.at[s, side(z)], rz.at[s, side(z)]
            elif paired:
                src, dst = sxz.at[s, side(z)], rxz.at[s, side(z)]
            else:
                src, dst = sxz.at[s, side(z), side(x)], rxz.at[s, side(z), side(x)]
        else:
            src = syz.at[s, side(z), side(y)]
            dst = ryz.at[s, side(z), side(y)]
        return pltpu.make_async_remote_copy(
            src_ref=src, dst_ref=dst, send_sem=send_sem.at[group(v)], recv_sem=recv_sem.at[s, group(v)],
            device_id=device(v),
        )

    def send(s, links):
        links = [v for v in links if not (paired and v[0] == -1)]
        for v in links:
            if v[2] == 0:
                message(s, v).start()
        for sign in SIDES:
            if any(v[2] == sign for v in links):
                @pl.when(has[sign])
                def _():
                    for v in links:
                        if v[2] == sign:
                            message(s, v).start()

    def rows(links):
        count = 0
        for x, y, z in links:
            if y == 0:
                count += FACE * ny if z == 0 else ny if x == 0 else 1
            else:
                count += FACE * nx if x == 0 and z == 0 else 1
        return count

    def settle(sem, count):
        pltpu.make_async_copy(ledger.at[0:count], ledger.at[0:count], sem).wait()

    def receive(s):
        settle(recv_sem.at[s, 0], rows(v for v in LINKS if v[2] == 0))
        for sign in SIDES:
            @pl.when(has[-sign])
            def _():
                settle(recv_sem.at[s, 1 + side(sign)], rows(v for v in LINKS if v[2] == sign))

    def flatten(sign, tile, at):
        column = jnp.broadcast_to(tile[:, at : at + 1], (ny, nz))
        return jnp.sum(jnp.where(slant[sign], column, 0.0), axis=0, keepdims=True)

    def target(x, q):
        return lax.rem(x + (LATTICE[q][0] + nx), nx) * FACE

    def keep_urgent(s, x, way, values):
        for j, q in enumerate(MEMBERS[0, way]):
            sx[s, side(way), j] = values[q]
        for y in SIDES:
            q = LATTICE.index((way, y, 0))
            r = ny - 1 if y == 1 else 0
            sxy[s, side(y), side(way)] = values[q][r : r + 1, :]

    def keep_plane(s, x, way, values, packs):
        for q in range(26):
            if LATTICE[q][0] != way:
                post[s, SLOT[q], x + 1] = values[q]
        for sign in SIDES:
            r = ny - 1 if sign == 1 else 0
            for j, q in enumerate(MEMBERS[1, sign]):
                if LATTICE[q][0] == way:
                    continue
                value = values[q]
                if LATTICE[q][2]:
                    value = pltpu.roll(value, LATTICE[q][2] % nz, 1)
                sy[s, side(sign), j, x + 1] = value[r : r + 1, :]
        new = []
        for sign, pack in zip(SIDES, packs):
            source = nz - 1 if sign == 1 else 0
            for j, q in enumerate(MEMBERS[2, sign]):
                k = target(x, q) + j
                turned = pltpu.roll(values[q], lax.rem(k + (nz - source), nz), 1)
                pack = jnp.where(lane == k, turned, pack)
            new.append(pack)
        return tuple(new)

    def stream(s, x):
        for q in range(26):
            cx, cy, cz = LATTICE[q]
            if cy or cz:
                value = post[s, SLOT[q], x + 1]
                if cz:
                    value = pltpu.roll(value, cz % nz, 1)
                if cy:
                    value = pltpu.roll(value, cy % ny, 0)
                mid[SLOT[q], x] = value

    def bounce(s, sign, pack, unit):
        own = MEMBERS[2, sign]
        edge = (nx - 1) * FACE
        wall = pack
        for x in SIDES:
            near_part = pltpu.roll(pack, (-x * FACE) % nz, 1)
            far_part = pltpu.roll(pack, (x * edge) % nz, 1)
            far = lane >= edge if x == 1 else lane < FACE
            wall = jnp.where(
                lanes_of(sign, lambda q: LATTICE[q][0] == x), jnp.where(far, far_part, near_part), wall
            )
        for y in SIDES:
            wall = jnp.where(
                lanes_of(sign, lambda q: LATTICE[q][1] == y), pltpu.roll(pack, -y % ny, 0), wall
            )
        weight = WEIGHTS[own[-1]]
        warm = (2.0 * weight * (COLD_WALL if sign == 1 else HOT_WALL)) * unit
        wall = jnp.where(lanes_of(sign, lambda q: q >= 19), warm - wall, wall)
        rz[s, side(-sign)] = wall
        for x in SIDES:
            q = LATTICE.index((x, 0, -sign))
            at = (0 if x == 1 else nx - 1) * FACE + MEMBERS[2, -sign].index(q)
            rxz[s, side(-sign), side(x)] = flatten(-sign, wall, at)

    def arrive():
        planes = ((0, cur.at[:, 0]), (1, cur.at[:, nx - 1]), (2, cur.at[:, 1 : nx - 1]))
        for part, planes_of in planes:
            pltpu.make_async_copy(planes_of, planes_of, in_sem.at[part]).wait()
            if part:
                yield

    def advance(s, body, arrive, before_send, unit):
        zero = jnp.zeros((ny, nz), jnp.float32)
        packs = (zero, zero)
        stages = iter(arrive() or ())
        next(stages, None)
        first = []
        for x, way in ((0, -1), (nx - 1, 1)):
            values = body(x, x)
            first.append((x, way, values))
            keep_urgent(s, x, way, values)
        before_send()
        send(s, [v for v in EARLY if v[1]])
        send(s, [v for v in EARLY if not v[1] and not v[2]])
        for x, way, values in first:
            for sign in SIDES:
                value = values[LATTICE.index((way, 0, sign))]
                sxz[s, side(sign), side(way)] = flatten(sign, value, nz - 1 if sign == 1 else 0)
        send(s, [v for v in EARLY if v[2]])
        for x, way, values in first:
            packs = keep_plane(s, x, way, values, packs)
        next(stages, None)
        packs = lax.fori_loop(
            1, nx - 1, lambda x, p: keep_plane(s, x, None, body(x, None), p), packs, unroll=UNROLL
        )
        send(s, [v for v in LATE if v[2] == 0])
        for sign, pack in zip(SIDES, packs):
            whole = pack
            for y in SIDES:
                whole = jnp.where(
                    lanes_of(sign, lambda q: LATTICE[q][1] == y), pltpu.roll(pack, y % ny, 0), whole
                )
            sz[s, side(sign)] = whole
            for y in SIDES:
                r = 0 if y == 1 else ny - 1
                syz[s, side(sign), side(y)] = whole[r : r + 1, :]
        send(s, [v for v in LATE if v[2]])
        for sign in SIDES:
            @pl.when(jnp.logical_not(has[sign]))
            def _():
                bounce(s, sign, sz[s, side(sign)], unit)
        lax.fori_loop(0, nx, lambda x, c: (stream(s, x), c)[1], 0, unroll=2)

    def columns(s):
        result = {}
        for sign in SIDES:
            tile = rz[s, side(sign)]
            for y in SIDES:
                mask = lanes_of(sign, lambda q: LATTICE[q][1] == y) & (first_row if y == 1 else last_row)
                edge = jnp.broadcast_to(ryz[s, side(sign), side(y)], (ny, nz))
                tile = jnp.where(mask & has[-sign], edge, tile)
            result[sign] = tile
        return result

    def pull(s, x, fixed, beyond, q):
        cx, cy, cz = LATTICE[q]
        at = x - cx + 1
        if fixed is not None and fixed - cx in (-1, nx):
            value = rx[s, side(cx), MEMBERS[0, cx].index(q)]
            if cz:
                value = pltpu.roll(value, cz % nz, 1)
            if cy:
                value = pltpu.roll(value, cy % ny, 0)
        elif cy or cz:
            value = mid[SLOT[q], at - 1]
        else:
            value = post[s, SLOT[q], at]
        if cy:
            j = MEMBERS[1, cy].index(q)
            if fixed is not None and fixed - cx in (-1, nx):
                line = rxy[s, side(cy), side(cx)]
            else:
                line = ry[s, side(cy), j, at]
            edge = jnp.broadcast_to(line, (ny, nz))
            value = jnp.where(first_row if cy == 1 else last_row, edge, value)
        if cz:
            j = MEMBERS[2, cz].index(q)
            end = 0 if cz == 1 else nz - 1
            if fixed is not None and fixed - cx in (-1, nx):
                line = jnp.broadcast_to(rxz[s, side(cz), side(cx)], (ny, nz))
                outer = pltpu.roll(line, 0, 1, stride=1, stride_axis=0)
            else:
                outer = pltpu.roll(beyond[cz], lax.rem(end + nz - (x * FACE + j), nz), 1)
            value = jnp.where(first_lane if cz == 1 else last_lane, outer, value)
        return value

    def fresh(x, fixed):
        return collide([cur[q, x] for q in range(19)], [cur[q, x] for q in range(19, 26)], 1.0)

    advance(0, fresh, arrive, greet, 1.0 / KEEP_HEAT)

    def step(s, carry):
        scale, unit = carry
        receive(s)
        beyond = columns(s)

        def body(x, fixed):
            values = [pull(s, x, fixed, beyond, q) for q in range(26)]
            return collide(values[:19], values[19:], scale)

        unit = unit * (1.0 / KEEP_HEAT)
        advance(s + 1, body, lambda: None, lambda: None, unit)
        return scale * KEEP_HEAT, unit

    lax.fori_loop(0, STEPS - 1, step, (jnp.float32(KEEP_HEAT), jnp.float32(1.0 / KEEP_HEAT)))

    last = STEPS - 1
    receive(last)
    beyond = columns(last)

    def finish(x, fixed, flux):
        values = [pull(last, x, fixed, beyond, q) for q in range(26)]
        for q in range(26):
            result[q, x] = (KEEP_FLOW if q < 19 else KEEP_HEAT) ** STEPS * values[q]
        _, warmth, _, u = moments(values[:19], values[19:], KEEP_HEAT**STEPS)
        return flux + u[2] * warmth

    flux = jnp.zeros((ny, nz), jnp.float32)
    for x in (0, nx - 1):
        flux = finish(x, x, flux)
    flux = lax.fori_loop(1, nx - 1, lambda x, t: finish(x, None, t), flux, unroll=UNROLL)
    sums[me] = jnp.sum(flux, axis=0, keepdims=True)

    def send_sum(target):
        pltpu.make_async_remote_copy(
            src_ref=sums.at[me], dst_ref=sums.at[me],
            send_sem=sum_send, recv_sem=sum_recv, device_id=target,
        ).start()

    if joined:
        xs, ys = ([lax.rem(at + d, n) for d in range(n)] for at, n in zip((gx, gy), sizes))
        for k in range(count_z):
            z = jnp.where(2 * gz >= count_z, k, count_z - 1 - k)
            for dx in reversed(range(count_x)):
                for dy in reversed(range(count_y)):
                    there = {"gx": xs[dx], "gy": ys[dy], "gz": z}
                    if dx or dy:
                        send_sum(there)
                    else:
                        pl.when(z != gz)(functools.partial(send_sum, there))
    else:
        pl.loop(1, everyone)(lambda d: send_sum(ahead(d)))

    settle(send_sem.at[0], STEPS * rows(v for v in LINKS if v[2] == 0))
    for sign in SIDES:
        @pl.when(has[sign])
        def _():
            settle(send_sem.at[1 + side(sign)], STEPS * rows(v for v in LINKS if v[2] == sign))
    all_rows = pltpu.make_async_remote_copy(
        src_ref=sums.at[pl.ds(0, everyone - 1)], dst_ref=sums.at[pl.ds(0, everyone - 1)],
        send_sem=sum_send, recv_sem=sum_recv, device_id=ahead(1),
    )
    all_rows.wait_send()
    all_rows.wait_recv()
    result[26, 0, 0:1, :] = jnp.sum(sums[...], axis=0)


def write_out(scale, result, flow_out, heat_out, nusselt_out, small, sem):
    flow_cuts, heat_cuts = (0, 4, 8, 12, 16, 19), (0, 4, 7)
    for a, b in zip(flow_cuts, flow_cuts[1:]):
        pltpu.make_async_copy(result.at[a:b], flow_out.at[a:b], sem.at[0]).start()
    for a, b in zip(heat_cuts, heat_cuts[1:]):
        pltpu.make_async_copy(result.at[19 + a : 19 + b], heat_out.at[a:b], sem.at[0]).start()
    small[...] = 1.0 + scale * jnp.sum(result[26, 0, 0:1, :], axis=1, keepdims=True)
    number = pltpu.make_async_copy(small, nusselt_out, sem.at[1])
    number.start()
    pltpu.make_async_copy(result.at[0:26], result.at[0:26], sem.at[0]).wait()
    number.wait()


def per_device(sizes, flow_pops, heat_pops):
    nx, ny, nz = flow_pops.shape[1:]
    count_x, count_y, count_z = sizes
    f32 = jnp.float32
    dma = pltpu.SemaphoreType.DMA
    cells = nx * ny * nz * count_x * count_y * count_z
    scale = nz * count_z / (DIFFUSIVITY * (HOT_WALL - COLD_WALL)) / cells * KEEP_HEAT**STEPS
    hbm = pl.BlockSpec(memory_space=pltpu.HBM)
    vmem = pl.BlockSpec(memory_space=pltpu.VMEM)
    result = pl.pallas_call(
        functools.partial(kernel, sizes),
        out_shape=pltpu.VMEM((27, nx, ny, nz), f32),
        in_specs=[hbm, hbm],
        out_specs=vmem,
        scratch_shapes=[
            pltpu.VMEM((26, nx, ny, nz), f32),
            pltpu.VMEM((STEPS, 26, nx + 2, ny, nz), f32),
            pltpu.VMEM((26, nx, ny, nz), f32),
            pltpu.VMEM((STEPS, 2, FACE, ny, nz), f32),
            pltpu.VMEM((STEPS, 2, FACE, ny, nz), f32),
            pltpu.VMEM((STEPS, 2, FACE, nx + 2, 1, nz), f32),
            pltpu.VMEM((STEPS, 2, FACE, nx + 2, 1, nz), f32),
            pltpu.VMEM((STEPS, 2, ny, nz), f32),
            pltpu.VMEM((STEPS, 2, ny, nz), f32),
            pltpu.VMEM((STEPS, 2, 2, 1, nz), f32),
            pltpu.VMEM((STEPS, 2, 2, 1, nz), f32),
            pltpu.VMEM((STEPS, 2, 2, 1, nz), f32),
            pltpu.VMEM((STEPS, 2, 2, 1, nz), f32),
            pltpu.VMEM((STEPS, 2, 2, 1, nz), f32),
            pltpu.VMEM((STEPS, 2, 2, 1, nz), f32),
            pltpu.VMEM((count_x * count_y * count_z, 1, nz), f32),
            pltpu.VMEM((STEPS * 2 * (FACE * (nx + ny) + 2), 1, nz), f32),
            dma((3,)),
            dma((3,)),
            dma((STEPS, 3)),
            dma,
            dma,
        ],
        compiler_params=pltpu.CompilerParams(
            collective_id=0, has_side_effects=True, vmem_limit_bytes=55000000
        ),
    )(pltpu.with_memory_space_constraint(flow_pops, pltpu.HBM), pltpu.with_memory_space_constraint(heat_pops, pltpu.HBM))
    flow, heat, nusselt = pl.pallas_call(
        functools.partial(write_out, scale),
        out_shape=(
            jax.ShapeDtypeStruct(flow_pops.shape, f32),
            jax.ShapeDtypeStruct(heat_pops.shape, f32),
            jax.ShapeDtypeStruct((1, 1), f32),
        ),
        in_specs=[vmem],
        out_specs=(hbm, hbm, hbm),
        scratch_shapes=[pltpu.VMEM((1, 1), f32), dma((2,))],
        compiler_params=pltpu.CompilerParams(vmem_limit_bytes=1024 * 1024),
    )(result)
    return flow, heat, nusselt.reshape(())


def solution(mesh):
    placed = P(None, "gx", "gy", "gz")
    sizes = tuple(mesh.shape[a] for a in ("gx", "gy", "gz"))
    return jax.shard_map(
        functools.partial(per_device, sizes),
        mesh=mesh,
        in_specs=(placed, placed),
        out_specs=(placed, placed, P()),
        check_vma=False,
    )
```
